8 devices in a mesh: dp: 8 (over z, y, x, core).
Axes of the slice: x: 2, y: 2, z: 1, core: 2. Of those that a mesh axis runs over, the one named last changes fastest.
Arguments:
- local_grads: bfloat16 [8, 49152, 768], P('dp')
- master: float32 [49152, 768], P('dp')
- mom_first: float32 [49152, 768], P('dp')
- mom_second: float32 [49152, 768], P('dp')
- learn_rate: float32 [], replicated
Outputs:
- output 1: float32 [49152, 768], P('dp')
- output 2: float32 [49152, 768], P('dp')
- output 3: float32 [49152, 768], P('dp')
- output 4: bfloat16 [49152, 768], replicated
All inputs are finite; a program needn't handle non-finite values.
Results may differ from the reference program's by a relative error of at most 0.001.
Values are sent between devices in bfloat16 or wider.
A program may use at most 1 GiB of HBM per device.

```python
import math
import jax
import jax.numpy as jnp
import numpy as np
from jax import lax

D = 768
ROWS_DEV = 6144
DEVICES = 8
LAYERS = 2
MIX_RANK = 32
DECAY_RANK = 64
ADAM_STEP = 10


def rule_table(model_width, total_rows):
    ffn_width = 7 * model_width // 2
    layer_rows = 6 * model_width + 2 * ffn_width + 16 + 10 * MIX_RANK + 2 * DECAY_RANK
    vocab_rows = (total_rows - LAYERS * layer_rows - 4) // 2
    base_rule = (1.0, 0.0)
    decay_rule = (1.0, 0.1)
    time_rule = (2.0, 0.0)
    pieces = [(vocab_rows, decay_rule)]
    for layer_idx in range(LAYERS):
        lead_rows = 12 if layer_idx == 0 else 10
        pieces = pieces + [(lead_rows + 10 * MIX_RANK, base_rule), (1, time_rule), (2 * DECAY_RANK, base_rule), (1, time_rule), (5 * model_width, decay_rule), (4, base_rule), (2 * ffn_width + model_width, decay_rule)]
    pieces = pieces + [(2, base_rule), (vocab_rows, decay_rule)]
    run_lengths = np.array([run_len for run_len, run_rule in pieces])
    lr_factor = np.repeat(np.array([run_rule[0] for run_len, run_rule in pieces]), run_lengths)
    decay_rate = np.repeat(np.array([run_rule[1] for run_len, run_rule in pieces]), run_lengths)
    return lr_factor, decay_rate


def setup_inputs(seed: int = 0) -> dict:
    key_grad, key_master, key_first, key_second, key_rate = jax.random.split(jax.random.key(seed), 5)
    total_rows = DEVICES * ROWS_DEV
    elem_count = total_rows * D
    grad_scale = 3.0 * math.sqrt(DEVICES / elem_count)
    clip_unit = 1.0 / math.sqrt(elem_count)

    def draw_device(dev_key):
        gauss_noise = jax.random.normal(dev_key, (total_rows, D), jnp.float32)
        return (grad_scale * gauss_noise).astype(jnp.bfloat16)

    local_grads = lax.map(draw_device, jax.random.split(key_grad, DEVICES))
    master = (0.5 / math.sqrt(D)) * jax.random.normal(key_master, (total_rows, D), jnp.float32)
    mom_first = 0.1 * clip_unit * jax.random.normal(key_first, (total_rows, D), jnp.float32)
    mom_second = jnp.square(0.1 * clip_unit * jax.random.uniform(key_second, (total_rows, D), jnp.float32, 0.5, 1.5))
    learn_rate = jax.random.uniform(key_rate, (), jnp.float32, 0.005, 0.015)
    return {'local_grads': local_grads, 'master': master, 'mom_first': mom_first, 'mom_second': mom_second, 'learn_rate': learn_rate}


def reference(local_grads, master, mom_first, mom_second, learn_rate):
    def add_device(running, grad_block):
        return running + grad_block.astype(jnp.float32), None

    grad_total = lax.scan(add_device, jnp.zeros(master.shape, jnp.float32), local_grads)[0]
    grad_mean = grad_total / local_grads.shape[0]
    grad_norm = jnp.sqrt(jnp.sum(grad_mean * grad_mean))
    clip_scale = jnp.minimum(1.0, 1.0 / (grad_norm + 1e-6))
    clipped = grad_mean * clip_scale
    new_first = 0.9 * mom_first + 0.1 * clipped
    new_second = 0.99 * mom_second + 0.01 * (clipped * clipped)
    first_hat = new_first / (1.0 - 0.9 ** ADAM_STEP)
    second_hat = new_second / (1.0 - 0.99 ** ADAM_STEP)
    lr_factor, decay_rate = rule_table(master.shape[1], master.shape[0])
    row_rate = learn_rate * jnp.asarray(lr_factor, jnp.float32)[:, None]
    row_decay = jnp.asarray(decay_rate, jnp.float32)[:, None]
    new_master = master - row_rate * (first_hat / (jnp.sqrt(second_hat) + 1e-8) + row_decay * master)
    return new_master, new_first, new_second, new_master.astype(jnp.bfloat16)
```

```python
import functools

import jax
import jax.numpy as jnp
from jax import lax
from jax.experimental import pallas as pl
from jax.experimental.pallas import tpu as pltpu
from jax.sharding import PartitionSpec as P

LAYERS = 2
MIX_RANK = 32
DECAY_RANK = 64
ADAM_STEP = 10
MESH = pl.DeviceIdType.MESH
TILE = 256
SLAB = 32


def layout_runs(model_width, total_rows):
    ffn_width = 7 * model_width // 2
    layer_rows = 6 * model_width + 2 * ffn_width + 16 + 10 * MIX_RANK + 2 * DECAY_RANK
    vocab_rows = (total_rows - LAYERS * layer_rows - 4) // 2
    base_rule = (1.0, 0.0)
    decay_rule = (1.0, 0.1)
    time_rule = (2.0, 0.0)
    pieces = [(vocab_rows, decay_rule)]
    for layer_idx in range(LAYERS):
        lead_rows = 12 if layer_idx == 0 else 10
        pieces = pieces + [(lead_rows + 10 * MIX_RANK, base_rule), (1, time_rule), (2 * DECAY_RANK, base_rule), (1, time_rule), (5 * model_width, decay_rule), (4, base_rule), (2 * ffn_width + model_width, decay_rule)]
    pieces = pieces + [(2, base_rule), (vocab_rows, decay_rule)]
    run_starts = []
    next_row = 0
    for run_len, run_rule in pieces:
        run_starts.append(next_row)
        next_row = next_row + run_len
    lr_values = [run_rule[0] for run_len, run_rule in pieces]
    decay_values = [run_rule[1] for run_len, run_rule in pieces]
    return run_starts, lr_values, decay_values


def row_rules(row_ids, model_width, total_rows):
    run_starts, lr_values, decay_values = layout_runs(model_width, total_rows)
    later_starts = jnp.asarray(run_starts[1:], jnp.int32)
    run_index = jnp.sum((row_ids[:, None] >= later_starts[None, :]).astype(jnp.int32), axis=1)
    lr_factor = jnp.asarray(lr_values, jnp.float32)[run_index]
    decay_rate = jnp.asarray(decay_values, jnp.float32)[run_index]
    return lr_factor[:, None], decay_rate[:, None]


def adam_rows(grad_rows, master_rows, first_rows, second_rows, clip_scale, learn_rate, lr_factor, decay_rate):
    clipped = grad_rows * clip_scale
    new_first = 0.9 * first_rows + 0.1 * clipped
    new_second = 0.99 * second_rows + 0.01 * (clipped * clipped)
    first_hat = new_first / (1.0 - 0.9 ** ADAM_STEP)
    second_hat = new_second / (1.0 - 0.99 ** ADAM_STEP)
    step_size = learn_rate * lr_factor
    new_master = master_rows - step_size * (first_hat / (jnp.sqrt(second_hat) + 1e-8) + decay_rate * master_rows)
    return new_master, new_first, new_second


def places():
    me = lax.axis_index('dp')
    core = me % 2
    x = (me // 2) % 2
    y = me // 4
    x_chip = y * 2 + (1 - x)
    y_chip = (1 - y) * 2 + x
    d_chip = (1 - y) * 2 + (1 - x)
    return me, core, me + 1 - 2 * core, x_chip, y_chip, d_chip


def greet(partners):
    barrier = pltpu.get_barrier_semaphore()
    for partner in partners:
        pl.semaphore_signal(barrier, inc=1, device_id=(partner,), device_id_type=MESH)
    pl.semaphore_wait(barrier, len(partners))


def reduce_kernel(shard, grads, total_ref, clip_ref, x_raw, y_raw, mate_raw, x_sum, y_sum,
                  relay, blocks, sums, finals, squares, norm_mine, norm_all,
                  x_sent, y_sent, mate_sent, xs_sent, ys_sent, x_got, y_got, mate_got, xs_got, ys_got,
                  load_sem, store_sem, norm_sent, norm_got):
    half = shard // 2
    tiles = half // TILE
    me, core, mate, x_chip, y_chip, d_chip = places()
    mate_core = 1 - core
    x_peer, y_peer, d_peer = x_chip * 2 + core, y_chip * 2 + core, d_chip * 2 + core
    everyone = [mate, x_chip * 2, x_chip * 2 + 1, y_chip * 2, y_chip * 2 + 1, d_chip * 2, d_chip * 2 + 1]
    greet(everyone)

    def rows(tile):
        return pl.ds(pl.multiple_of(tile * TILE, TILE), TILE)

    def grad_tile(owner, part, tile):
        return grads.at[0, pl.ds(pl.multiple_of(owner * shard + part * half + tile * TILE, TILE), TILE), :]

    def remote(src, dst, sent, got, device):
        return pltpu.make_async_remote_copy(src_ref=src, dst_ref=dst, send_sem=sent, recv_sem=got, device_id=(device,), device_id_type=MESH)

    def send_raw(stage, tile):
        x_owner = d_chip if stage == 0 else x_chip
        y_owner = d_chip if stage == 0 else y_chip
        for dest in range(2):
            remote(grad_tile(x_owner * 2 + dest, 0, tile), x_raw.at[stage, core, rows(tile)], x_sent.at[tile], x_got.at[stage, core, tile], x_chip * 2 + dest).start()
            remote(grad_tile(y_owner * 2 + dest, 1, tile), y_raw.at[stage, core, rows(tile)], y_sent.at[tile], y_got.at[stage, core, tile], y_chip * 2 + dest).start()
        first = y_chip * 2 + mate_core if stage == 0 else mate
        second = x_chip * 2 + mate_core if stage == 0 else mate
        remote(grad_tile(first, 0, tile), mate_raw.at[2 * stage, rows(tile)], mate_sent.at[tile], mate_got.at[2 * stage, tile], mate).start()
        remote(grad_tile(second, 1, tile), mate_raw.at[2 * stage + 1, rows(tile)], mate_sent.at[tile], mate_got.at[2 * stage + 1, tile], mate).start()

    def arrived(ref, sem):
        remote(ref, ref, sem, sem, mate).wait_recv()

    def wait_raw(stage, tile):
        for source in range(2):
            arrived(x_raw.at[stage, source, rows(tile)], x_got.at[stage, source, tile])
            arrived(y_raw.at[stage, source, rows(tile)], y_got.at[stage, source, tile])
        for part in range(2):
            arrived(mate_raw.at[2 * stage + part, rows(tile)], mate_got.at[2 * stage + part, tile])

    def loads(stage, tile):
        owners = (y_peer, x_peer) if stage == 0 else (me, me)
        out = []
        for part in range(2):
            far = x_raw if part == 0 else y_raw
            sources = [grad_tile(owners[part], part, tile), mate_raw.at[2 * stage + part, rows(tile)], far.at[stage, 0, rows(tile)], far.at[stage, 1, rows(tile)]]
            for k, source in enumerate(sources):
                out.append(pltpu.make_async_copy(source, blocks.at[part, k], load_sem.at[part, k]))
        return out

    @pl.loop(0, tiles)
    def _(tile):
        send_raw(0, tile)

    @pl.loop(0, tiles)
    def _(tile):
        send_raw(1, tile)
        wait_raw(0, tile)
        copies = loads(0, tile)
        for copy in copies:
            copy.start()
        for part in range(2):
            for copy in copies[4 * part:4 * part + 4]:
                copy.wait()

            @pl.loop(0, TILE // SLAB)
            def _(slab):
                at = pl.ds(pl.multiple_of(slab * SLAB, SLAB), SLAB)
                parts = [blocks[part, k, at, :].astype(jnp.float32) for k in range(4)]
                relay[part, tile, at, :] = (parts[0] + parts[1]) + (parts[2] + parts[3])

            if part == 0:
                remote(relay.at[0, tile], y_sum.at[rows(tile)], ys_sent.at[tile], ys_got.at[tile], y_peer).start()
            else:
                remote(relay.at[1, tile], x_sum.at[rows(tile)], xs_sent.at[tile], xs_got.at[tile], x_peer).start()

    squares[...] = jnp.zeros_like(squares)

    def total_tile(part, tile):
        return total_ref.at[pl.ds(pl.multiple_of(part * half + tile * TILE, TILE), TILE), :]

    @pl.loop(0, tiles)
    def _(tile):
        wait_raw(1, tile)
        copies = loads(1, tile)
        for copy in copies:
            copy.start()
        arrived(y_sum.at[rows(tile)], ys_got.at[tile])
        first_sum = pltpu.make_async_copy(y_sum.at[rows(tile)], sums.at[0], load_sem.at[0, 4])
        first_sum.start()
        arrived(x_sum.at[rows(tile)], xs_got.at[tile])
        second_sum = pltpu.make_async_copy(x_sum.at[rows(tile)], sums.at[1], load_sem.at[1, 4])
        second_sum.start()
        for part in range(2):
            for copy in copies[4 * part:4 * part + 4]:
                copy.wait()
            (first_sum, second_sum)[part].wait()

            @pl.when(tile > 0)
            def _():
                pltpu.make_async_copy(finals.at[part], total_tile(part, tile), store_sem.at[part]).wait()

            @pl.loop(0, TILE // SLAB)
            def _(slab):
                at = pl.ds(pl.multiple_of(slab * SLAB, SLAB), SLAB)
                parts = [blocks[part, k, at, :].astype(jnp.float32) for k in range(4)]
                mean = ((parts[0] + parts[1]) + (parts[2] + parts[3]) + sums[part, at, :]) * 0.125
                finals[part, at, :] = mean
                squares[...] += jnp.sum((mean * mean).reshape(SLAB // 8, 8, mean.shape[1]), axis=0)

            pltpu.make_async_copy(finals.at[part], total_tile(part, tile), store_sem.at[part]).start()

    width = squares.shape[1]
    packed = squares[:, 0:128]
    for lane in range(1, width // 128):
        packed = packed + squares[:, lane * 128:lane * 128 + 128]
    norm_mine[...] = packed
    norm_all[me] = packed
    for part in range(2):
        pltpu.make_async_copy(finals.at[part], total_tile(part, 0), store_sem.at[part]).wait()
    for k, partner in enumerate(everyone):
        remote(norm_mine, norm_all.at[me], norm_sent.at[k], norm_got.at[me], partner).start()
    for k, partner in enumerate(everyone):
        arrived(norm_all.at[partner], norm_got.at[partner])
    squared = norm_all[0]
    for k in range(1, 8):
        squared = squared + norm_all[k]
    norm = jnp.sqrt(jnp.sum(squared))
    clip_ref[...] = jnp.broadcast_to(jnp.minimum(1.0, 1.0 / (norm + 1e-6)), clip_ref.shape)

    for k, partner in enumerate(everyone):
        remote(norm_mine, norm_mine, norm_sent.at[k], norm_sent.at[k], partner).wait_send()

    @pl.loop(0, tiles)
    def _(tile):
        for ref, sem in ((x_raw.at[:, :, rows(tile)], x_sent), (y_raw.at[:, :, rows(tile)], y_sent), (mate_raw.at[:, rows(tile)], mate_sent),
                         (x_sum.at[rows(tile)], xs_sent), (y_sum.at[rows(tile)], ys_sent)):
            remote(ref, ref, sem.at[tile], sem.at[tile], mate).wait_send()


def reduce_grads(local_grads, shard):
    width = local_grads.shape[2]
    half = shard // 2
    tiles = half // TILE
    any_spec = pl.BlockSpec(memory_space=pl.ANY)
    bf16, f32 = jnp.bfloat16, jnp.float32
    dma = pltpu.SemaphoreType.DMA
    outs = pl.pallas_call(
        functools.partial(reduce_kernel, shard),
        out_shape=[
            jax.ShapeDtypeStruct((shard, width), f32),
            jax.ShapeDtypeStruct((8, 128), f32),
            jax.ShapeDtypeStruct((2, 2, half, width), bf16),
            jax.ShapeDtypeStruct((2, 2, half, width), bf16),
            jax.ShapeDtypeStruct((4, half, width), bf16),
            jax.ShapeDtypeStruct((half, width), f32),
            jax.ShapeDtypeStruct((half, width), f32),
        ],
        in_specs=[any_spec],
        out_specs=[any_spec, pl.BlockSpec(memory_space=pltpu.VMEM)] + [any_spec] * 5,
        scratch_shapes=[
            pltpu.VMEM((2, tiles, TILE, width), f32),
            pltpu.VMEM((2, 4, TILE, width), bf16),
            pltpu.VMEM((2, TILE, width), f32),
            pltpu.VMEM((2, TILE, width), f32),
            pltpu.VMEM((8, width), f32),
            pltpu.VMEM((8, 128), f32),
            pltpu.VMEM((8, 8, 128), f32),
            dma((tiles,)), dma((tiles,)), dma((tiles,)), dma((tiles,)), dma((tiles,)),
            dma((2, 2, tiles)), dma((2, 2, tiles)), dma((4, tiles)), dma((tiles,)), dma((tiles,)),
            dma((2, 5)), dma((2,)), dma((7,)), dma((8,)),
        ],
        compiler_params=pltpu.CompilerParams(collective_id=0, has_side_effects=True, vmem_limit_bytes=56 * 2 ** 20),
        name='reduce_grads',
    )(local_grads)
    return outs[0], outs[1]


def solution(mesh):
    dev_count = mesh.shape['dp']

    def device_step(local_grads, master, mom_first, mom_second, learn_rate):
        shard_rows = master.shape[0]
        model_width = master.shape[1]
        total_rows = shard_rows * dev_count
        grad_shard, clip = reduce_grads(local_grads, shard_rows)
        clip_scale = clip[0, 0]
        row_ids = lax.axis_index('dp') * shard_rows + lax.iota(jnp.int32, shard_rows)
        lr_factor, decay_rate = row_rules(row_ids, model_width, total_rows)
        new_master, new_first, new_second = adam_rows(grad_shard, master, mom_first, mom_second, clip_scale, learn_rate, lr_factor, decay_rate)
        working = lax.all_gather(new_master.astype(jnp.bfloat16), 'dp', axis=0, tiled=True)
        return new_master, new_first, new_second, working

    return jax.shard_map(device_step, mesh=mesh, in_specs=(P('dp', None, None), P('dp', None), P('dp', None), P('dp', None), P()), out_specs=(P('dp', None), P('dp', None), P('dp', None), P(None, None)), check_vma=False)
```

```python
import functools

import jax
import jax.numpy as jnp
from jax import lax
from jax.experimental import pallas as pl
from jax.experimental.pallas import tpu as pltpu
from jax.sharding import PartitionSpec as P

LAYERS = 2
MIX_RANK = 32
DECAY_RANK = 64
ADAM_STEP = 10
MESH = pl.DeviceIdType.MESH
TILE = 256
SLAB = 32
ADAM_TILE = 192
ADAM_SLAB = 32
CHUNKS = (384, 384, 768, 768, 1152, 1152, 768, 768)
ADAM_FLOPS = 60
PLACE_FLOPS = 16


def layout_runs(model_width, total_rows):
    ffn_width = 7 * model_width // 2
    layer_rows = 6 * model_width + 2 * ffn_width + 16 + 10 * MIX_RANK + 2 * DECAY_RANK
    vocab_rows = (total_rows - LAYERS * layer_rows - 4) // 2
    base_rule = (1.0, 0.0)
    decay_rule = (1.0, 0.1)
    time_rule = (2.0, 0.0)
    pieces = [(vocab_rows, decay_rule)]
    for layer_idx in range(LAYERS):
        lead_rows = 12 if layer_idx == 0 else 10
        pieces = pieces + [(lead_rows + 10 * MIX_RANK, base_rule), (1, time_rule), (2 * DECAY_RANK, base_rule), (1, time_rule), (5 * model_width, decay_rule), (4, base_rule), (2 * ffn_width + model_width, decay_rule)]
    pieces = pieces + [(2, base_rule), (vocab_rows, decay_rule)]
    run_starts = []
    next_row = 0
    for run_len, run_rule in pieces:
        run_starts.append(next_row)
        next_row = next_row + run_len
    lr_values = [run_rule[0] for run_len, run_rule in pieces]
    decay_values = [run_rule[1] for run_len, run_rule in pieces]
    return run_starts, lr_values, decay_values


def places():
    me = lax.axis_index('dp')
    core = me % 2
    x = (me // 2) % 2
    y = me // 4
    x_chip = y * 2 + (1 - x)
    y_chip = (1 - y) * 2 + x
    d_chip = (1 - y) * 2 + (1 - x)
    return me, core, me + 1 - 2 * core, x_chip, y_chip, d_chip


def greet(partners):
    barrier = pltpu.get_barrier_semaphore()
    for partner in partners:
        pl.semaphore_signal(barrier, inc=1, device_id=(partner,), device_id_type=MESH)
    pl.semaphore_wait(barrier, len(partners))


def reduce_kernel(shard, grads, total_ref, clip_ref, x_raw, y_raw, mate_raw, x_sum, y_sum,
                  relay, blocks, sums, finals, squares, norm_mine, norm_all,
                  x_sent, y_sent, mate_sent, xs_sent, ys_sent, x_got, y_got, mate_got, xs_got, ys_got,
                  load_sem, store_sem, norm_sent, norm_got):
    half = shard // 2
    tiles = half // TILE
    me, core, mate, x_chip, y_chip, d_chip = places()
    mate_core = 1 - core
    x_peer, y_peer = x_chip * 2 + core, y_chip * 2 + core
    everyone = [mate, x_chip * 2, x_chip * 2 + 1, y_chip * 2, y_chip * 2 + 1, d_chip * 2, d_chip * 2 + 1]
    greet(everyone)

    def rows(tile):
        return pl.ds(pl.multiple_of(tile * TILE, TILE), TILE)

    def grad_tile(owner, part, tile):
        return grads.at[0, pl.ds(pl.multiple_of(owner * shard + part * half + tile * TILE, TILE), TILE), :]

    def remote(src, dst, sent, got, device):
        return pltpu.make_async_remote_copy(src_ref=src, dst_ref=dst, send_sem=sent, recv_sem=got, device_id=(device,), device_id_type=MESH)

    def send_raw(stage, tile):
        x_owner = d_chip if stage == 0 else x_chip
        y_owner = d_chip if stage == 0 else y_chip
        for dest in range(2):
            remote(grad_tile(x_owner * 2 + dest, 0, tile), x_raw.at[stage, core, rows(tile)], x_sent.at[tile], x_got.at[stage, core, tile], x_chip * 2 + dest).start()
            remote(grad_tile(y_owner * 2 + dest, 1, tile), y_raw.at[stage, core, rows(tile)], y_sent.at[tile], y_got.at[stage, core, tile], y_chip * 2 + dest).start()
        first = y_chip * 2 + mate_core if stage == 0 else mate
        second = x_chip * 2 + mate_core if stage == 0 else mate
        remote(grad_tile(first, 0, tile), mate_raw.at[2 * stage, rows(tile)], mate_sent.at[tile], mate_got.at[2 * stage, tile], mate).start()
        remote(grad_tile(second, 1, tile), mate_raw.at[2 * stage + 1, rows(tile)], mate_sent.at[tile], mate_got.at[2 * stage + 1, tile], mate).start()

    def arrived(ref, sem):
        remote(ref, ref, sem, sem, mate).wait_recv()

    def wait_raw(stage, tile):
        for source in range(2):
            arrived(x_raw.at[stage, source, rows(tile)], x_got.at[stage, source, tile])
            arrived(y_raw.at[stage, source, rows(tile)], y_got.at[stage, source, tile])
        for part in range(2):
            arrived(mate_raw.at[2 * stage + part, rows(tile)], mate_got.at[2 * stage + part, tile])

    def loads(stage, tile):
        owners = (y_peer, x_peer) if stage == 0 else (me, me)
        out = []
        for part in range(2):
            far = x_raw if part == 0 else y_raw
            sources = [grad_tile(owners[part], part, tile), mate_raw.at[2 * stage + part, rows(tile)], far.at[stage, 0, rows(tile)], far.at[stage, 1, rows(tile)]]
            for k, source in enumerate(sources):
                out.append(pltpu.make_async_copy(source, blocks.at[part, k], load_sem.at[part, k]))
        return out

    @pl.loop(0, tiles)
    def _(tile):
        send_raw(0, tile)

    @pl.loop(0, tiles)
    def _(tile):
        send_raw(1, tile)
        wait_raw(0, tile)
        copies = loads(0, tile)
        for copy in copies:
            copy.start()
        for part in range(2):
            for copy in copies[4 * part:4 * part + 4]:
                copy.wait()

            @pl.loop(0, TILE // SLAB)
            def _(slab):
                at = pl.ds(pl.multiple_of(slab * SLAB, SLAB), SLAB)
                parts = [blocks[part, k, at, :].astype(jnp.float32) for k in range(4)]
                relay[part, tile, at, :] = (parts[0] + parts[1]) + (parts[2] + parts[3])

            if part == 0:
                remote(relay.at[0, tile], y_sum.at[rows(tile)], ys_sent.at[tile], ys_got.at[tile], y_peer).start()
            else:
                remote(relay.at[1, tile], x_sum.at[rows(tile)], xs_sent.at[tile], xs_got.at[tile], x_peer).start()

    squares[...] = jnp.zeros_like(squares)

    def total_tile(part, tile):
        return total_ref.at[pl.ds(pl.multiple_of(part * half + tile * TILE, TILE), TILE), :]

    @pl.loop(0, tiles)
    def _(tile):
        wait_raw(1, tile)
        copies = loads(1, tile)
        for copy in copies:
            copy.start()
        arrived(y_sum.at[rows(tile)], ys_got.at[tile])
        first_sum = pltpu.make_async_copy(y_sum.at[rows(tile)], sums.at[0], load_sem.at[0, 4])
        first_sum.start()
        arrived(x_sum.at[rows(tile)], xs_got.at[tile])
        second_sum = pltpu.make_async_copy(x_sum.at[rows(tile)], sums.at[1], load_sem.at[1, 4])
        second_sum.start()
        for part in range(2):
            for copy in copies[4 * part:4 * part + 4]:
                copy.wait()
            (first_sum, second_sum)[part].wait()

            @pl.when(tile > 0)
            def _():
                pltpu.make_async_copy(finals.at[part], total_tile(part, tile), store_sem.at[part]).wait()

            @pl.loop(0, TILE // SLAB)
            def _(slab):
                at = pl.ds(pl.multiple_of(slab * SLAB, SLAB), SLAB)
                parts = [blocks[part, k, at, :].astype(jnp.float32) for k in range(4)]
                mean = ((parts[0] + parts[1]) + (parts[2] + parts[3]) + sums[part, at, :]) * 0.125
                finals[part, at, :] = mean
                squares[...] += jnp.sum((mean * mean).reshape(SLAB // 8, 8, mean.shape[1]), axis=0)

            pltpu.make_async_copy(finals.at[part], total_tile(part, tile), store_sem.at[part]).start()

    width = squares.shape[1]
    packed = squares[:, 0:128]
    for lane in range(1, width // 128):
        packed = packed + squares[:, lane * 128:lane * 128 + 128]
    norm_mine[...] = packed
    norm_all[me] = packed
    for part in range(2):
        pltpu.make_async_copy(finals.at[part], total_tile(part, 0), store_sem.at[part]).wait()
    for k, partner in enumerate(everyone):
        remote(norm_mine, norm_all.at[me], norm_sent.at[k], norm_got.at[me], partner).start()
    for partner in everyone:
        arrived(norm_all.at[partner], norm_got.at[partner])
    squared = norm_all[0]
    for k in range(1, 8):
        squared = squared + norm_all[k]
    norm = jnp.sqrt(jnp.sum(squared))
    clip_ref[...] = jnp.broadcast_to(jnp.minimum(1.0, 1.0 / (norm + 1e-6)), clip_ref.shape)

    for k, partner in enumerate(everyone):
        remote(norm_mine, norm_mine, norm_sent.at[k], norm_sent.at[k], partner).wait_send()

    @pl.loop(0, tiles)
    def _(tile):
        for ref, sem in ((x_raw.at[:, :, rows(tile)], x_sent), (y_raw.at[:, :, rows(tile)], y_sent), (mate_raw.at[:, rows(tile)], mate_sent),
                         (x_sum.at[rows(tile)], xs_sent), (y_sum.at[rows(tile)], ys_sent)):
            remote(ref, ref, sem.at[tile], sem.at[tile], mate).wait_send()


def reduce_grads(local_grads, shard):
    width = local_grads.shape[2]
    half = shard // 2
    tiles = half // TILE
    any_spec = pl.BlockSpec(memory_space=pl.ANY)
    bf16, f32 = jnp.bfloat16, jnp.float32
    dma = pltpu.SemaphoreType.DMA
    outs = pl.pallas_call(
        functools.partial(reduce_kernel, shard),
        out_shape=[
            jax.ShapeDtypeStruct((shard, width), f32),
            jax.ShapeDtypeStruct((8, 128), f32),
            jax.ShapeDtypeStruct((2, 2, half, width), bf16),
            jax.ShapeDtypeStruct((2, 2, half, width), bf16),
            jax.ShapeDtypeStruct((4, half, width), bf16),
            jax.ShapeDtypeStruct((half, width), f32),
            jax.ShapeDtypeStruct((half, width), f32),
        ],
        in_specs=[any_spec],
        out_specs=[any_spec, pl.BlockSpec(memory_space=pltpu.VMEM)] + [any_spec] * 5,
        scratch_shapes=[
            pltpu.VMEM((2, tiles, TILE, width), f32),
            pltpu.VMEM((2, 4, TILE, width), bf16),
            pltpu.VMEM((2, TILE, width), f32),
            pltpu.VMEM((2, TILE, width), f32),
            pltpu.VMEM((8, width), f32),
            pltpu.VMEM((8, 128), f32),
            pltpu.VMEM((8, 8, 128), f32),
            dma((tiles,)), dma((tiles,)), dma((tiles,)), dma((tiles,)), dma((tiles,)),
            dma((2, 2, tiles)), dma((2, 2, tiles)), dma((4, tiles)), dma((tiles,)), dma((tiles,)),
            dma((2, 5)), dma((2,)), dma((7,)), dma((8,)),
        ],
        compiler_params=pltpu.CompilerParams(collective_id=0, has_side_effects=True, vmem_limit_bytes=56 * 2 ** 20),
        name='reduce_grads',
    )(local_grads)
    return outs[0], outs[1]


def adam_kernel(first_row, shard, total_rows, rate_ref, clip_ref, grad, master, first, second, *refs):
    new_master, new_first, new_second, rounded = refs[-4:]
    width = grad.shape[1]
    run_starts, lr_values, decay_values = layout_runs(width, total_rows)
    start = lax.axis_index('dp') * shard + first_row + pl.program_id(0) * ADAM_TILE
    rate = rate_ref[0]
    clip_scale = clip_ref[0:1, 0:1]

    @pl.loop(0, ADAM_TILE // ADAM_SLAB)
    def _(slab):
        at = pl.ds(pl.multiple_of(slab * ADAM_SLAB, ADAM_SLAB), ADAM_SLAB)
        row = start + slab * ADAM_SLAB + lax.broadcasted_iota(jnp.int32, (ADAM_SLAB, 128), 0)
        lr_factor = jnp.full((ADAM_SLAB, 128), lr_values[0], jnp.float32)
        decay = jnp.full((ADAM_SLAB, 128), decay_values[0], jnp.float32)
        for k in range(1, len(run_starts)):
            later = row >= run_starts[k]
            if lr_values[k] != lr_values[k - 1]:
                lr_factor = jnp.where(later, lr_values[k], lr_factor)
            if decay_values[k] != decay_values[k - 1]:
                decay = jnp.where(later, decay_values[k], decay)
        step_size = rate * lr_factor
        for lane in range(width // 128):
            cols = pl.ds(lane * 128, 128)
            clipped = grad[at, cols] * clip_scale
            old = master[at, cols]
            next_first = 0.9 * first[at, cols] + 0.1 * clipped
            next_second = 0.99 * second[at, cols] + 0.01 * (clipped * clipped)
            first_hat = next_first / (1.0 - 0.9 ** ADAM_STEP)
            second_hat = next_second / (1.0 - 0.99 ** ADAM_STEP)
            value = old - step_size * (first_hat / (jnp.sqrt(second_hat) + 1e-8) + decay * old)
            new_first[at, cols] = next_first
            new_second[at, cols] = next_second
            new_master[at, cols] = value
            rounded[at, cols] = value.astype(jnp.bfloat16)


def adam_chunk(first_row, chunk, rate, clip, grad, states, previous, total_rows):
    shard, width = grad.shape
    block = pl.BlockSpec((ADAM_TILE, width), lambda step: (first_row // ADAM_TILE + step, 0))
    own = pl.BlockSpec((ADAM_TILE, width), lambda step: (step, 0))
    any_spec = pl.BlockSpec(memory_space=pl.ANY)
    smem = pl.BlockSpec(memory_space=pltpu.SMEM)
    vmem = pl.BlockSpec((8, 128), lambda step: (0, 0))
    full = jax.ShapeDtypeStruct((shard, width), jnp.float32)
    return pl.pallas_call(
        functools.partial(adam_kernel, first_row, shard, total_rows),
        grid=(chunk // ADAM_TILE,),
        out_shape=[full] * 3 + [jax.ShapeDtypeStruct((chunk, width), jnp.bfloat16)],
        in_specs=[smem, vmem] + [block] * 4 + [any_spec] * len(previous),
        out_specs=[block] * 3 + [own],
        input_output_aliases={6 + k: k for k in range(len(previous))},
        compiler_params=pltpu.CompilerParams(vmem_limit_bytes=56 * 2 ** 20),
        cost_estimate=pl.CostEstimate(flops=ADAM_FLOPS * chunk * width, bytes_accessed=30 * chunk * width, transcendentals=0),
    )(rate, clip, grad, *states, *previous)


def place_kernel(count, shard, first_row, partners, *refs):
    pieces = refs[:count]
    target, held, loaded, stored = refs[-4:]
    me, core, _, x_chip, y_chip, d_chip = places()
    chips = {'m': me // 2, 'x': x_chip, 'y': y_chip, 'd': d_chip}
    rows = held.shape[1]
    for k in range(count):
        pltpu.make_async_copy(pieces[k], held.at[k], loaded.at[k]).start()

    def store(k):
        chip, far = partners[k]
        owner = chips[chip] * 2 + (core if far == 0 else 1 - core)
        at = pl.multiple_of(owner * shard + first_row, 128)
        return pltpu.make_async_copy(held.at[k], target.at[pl.ds(at, rows)], stored.at[k])

    for k in range(count):
        pltpu.make_async_copy(pieces[k], held.at[k], loaded.at[k]).wait()
        store(k).start()
    for k in range(count):
        store(k).wait()


def place(shard, first_row, labelled, target, total_rows):
    pieces = [piece for _, piece in labelled]
    partners = [label for label, _ in labelled]
    rows, width = pieces[0].shape
    count = len(pieces)
    any_spec = pl.BlockSpec(memory_space=pl.ANY)
    previous = [] if target is None else [target]
    return pl.pallas_call(
        functools.partial(place_kernel, count, shard, first_row, partners),
        out_shape=jax.ShapeDtypeStruct((total_rows, width), jnp.bfloat16),
        in_specs=[any_spec] * (count + len(previous)),
        out_specs=any_spec,
        scratch_shapes=[pltpu.VMEM((count, rows, width), jnp.bfloat16), pltpu.SemaphoreType.DMA((count,)), pltpu.SemaphoreType.DMA((count,))],
        input_output_aliases={count: 0} if previous else {},
        compiler_params=pltpu.CompilerParams(vmem_limit_bytes=56 * 2 ** 20),
        cost_estimate=pl.CostEstimate(flops=PLACE_FLOPS * count * rows * width, bytes_accessed=4 * count * rows * width, transcendentals=0),
    )(*pieces, *previous)


def swap(value, bit):
    return lax.ppermute(value, 'dp', [(i, i ^ bit) for i in range(8)])


def solution(mesh):
    dev_count = mesh.shape['dp']

    def device_step(local_grads, master, mom_first, mom_second, learn_rate):
        shard = master.shape[0]
        total_rows = shard * dev_count
        grad_shard, clip = reduce_grads(local_grads, shard)
        rate = learn_rate.reshape(1)
        previous = []
        chunks = []
        first_row = 0
        for chunk in CHUNKS:
            outs = adam_chunk(first_row, chunk, rate, clip, grad_shard, (master, mom_first, mom_second), previous, total_rows)
            previous = list(outs[:3])
            chunks.append((first_row, outs[3]))
            first_row += chunk
        target = None
        pieces = []
        for index, (first_row, mine) in enumerate(chunks):
            from_x = swap(mine, 2)
            from_y = swap(mine, 4)
            from_d = swap(from_x, 4) if index % 2 == 0 else swap(from_y, 2)
            near = [(('m', 0), mine), (('m', 1), swap(mine, 1)), (('x', 0), from_x), (('x', 1), swap(from_x, 1)), (('y', 0), from_y), (('y', 1), swap(from_y, 1))]
            far = [(('d', 0), from_d), (('d', 1), swap(from_d, 1))]
            pieces.append((first_row, near, far))
        for first_row, near, far in pieces:
            target = place(shard, first_row, near, target, total_rows)
        for first_row, near, far in pieces:
            target = place(shard, first_row, far, target, total_rows)
        return (*previous, target)

    return jax.shard_map(device_step, mesh=mesh, in_specs=(P('dp', None, None), P('dp', None), P('dp', None), P('dp', None), P()), out_specs=(P('dp', None), P('dp', None), P('dp', None), P(None, None)), check_vma=False)
```

```python
import functools

import jax
import jax.numpy as jnp
from jax import lax
from jax.experimental import pallas as pl
from jax.experimental.pallas import tpu as pltpu
from jax.sharding import PartitionSpec as P

LAYERS = 2
MIX_RANK = 32
DECAY_RANK = 64
ADAM_STEP = 10
MESH = pl.DeviceIdType.MESH
TILE = 256
SLAB = 32
ADAM_TILE = 192
ADAM_SLAB = 32
CHUNKS = (384, 384, 1152, 1152, 960, 960, 384, 384, 192, 192)
ADAM_FLOPS = 60
PLACE_FLOPS = 16
PLACE_VMEM = 24 * 2 ** 20


def layout_runs(model_width, total_rows):
    ffn_width = 7 * model_width // 2
    layer_rows = 6 * model_width + 2 * ffn_width + 16 + 10 * MIX_RANK + 2 * DECAY_RANK
    vocab_rows = (total_rows - LAYERS * layer_rows - 4) // 2
    base_rule = (1.0, 0.0)
    decay_rule = (1.0, 0.1)
    time_rule = (2.0, 0.0)
    pieces = [(vocab_rows, decay_rule)]
    for layer_idx in range(LAYERS):
        lead_rows = 12 if layer_idx == 0 else 10
        pieces = pieces + [(lead_rows + 10 * MIX_RANK, base_rule), (1, time_rule), (2 * DECAY_RANK, base_rule), (1, time_rule), (5 * model_width, decay_rule), (4, base_rule), (2 * ffn_width + model_width, decay_rule)]
    pieces = pieces + [(2, base_rule), (vocab_rows, decay_rule)]
    run_starts = []
    next_row = 0
    for run_len, run_rule in pieces:
        run_starts.append(next_row)
        next_row = next_row + run_len
    lr_values = [run_rule[0] for run_len, run_rule in pieces]
    decay_values = [run_rule[1] for run_len, run_rule in pieces]
    return run_starts, lr_values, decay_values


def places():
    me = lax.axis_index('dp')
    core = me % 2
    x = (me // 2) % 2
    y = me // 4
    x_chip = y * 2 + (1 - x)
    y_chip = (1 - y) * 2 + x
    d_chip = (1 - y) * 2 + (1 - x)
    return me, core, me + 1 - 2 * core, x_chip, y_chip, d_chip


def greet(partners):
    barrier = pltpu.get_barrier_semaphore()
    for partner in partners:
        pl.semaphore_signal(barrier, inc=1, device_id=(partner,), device_id_type=MESH)
    pl.semaphore_wait(barrier, len(partners))


def reduce_kernel(shard, grads, total_ref, clip_ref, x_raw, y_raw, mate_raw,
                  relay, blocks, x_sum, y_sum, finals, squares, norm_mine, norm_all,
                  x_sent, y_sent, mate_sent, xs_sent, ys_sent, x_got, y_got, mate_got, xs_got, ys_got,
                  load_sem, store_sem, norm_sent, norm_got):
    half = shard // 2
    tiles = half // TILE
    me, core, mate, x_chip, y_chip, d_chip = places()
    mate_core = 1 - core
    x_peer, y_peer = x_chip * 2 + core, y_chip * 2 + core
    everyone = [mate, x_chip * 2, x_chip * 2 + 1, y_chip * 2, y_chip * 2 + 1, d_chip * 2, d_chip * 2 + 1]
    greet(everyone)

    def rows(tile):
        return pl.ds(pl.multiple_of(tile * TILE, TILE), TILE)

    def grad_tile(owner, part, tile):
        return grads.at[0, pl.ds(pl.multiple_of(owner * shard + part * half + tile * TILE, TILE), TILE), :]

    def remote(src, dst, sent, got, device):
        return pltpu.make_async_remote_copy(src_ref=src, dst_ref=dst, send_sem=sent, recv_sem=got, device_id=(device,), device_id_type=MESH)

    def send_raw(stage, tile):
        x_owner = d_chip if stage == 0 else x_chip
        y_owner = d_chip if stage == 0 else y_chip
        for dest in range(2):
            remote(grad_tile(x_owner * 2 + dest, 0, tile), x_raw.at[stage, core, rows(tile)], x_sent.at[tile], x_got.at[stage, core, tile], x_chip * 2 + dest).start()
            remote(grad_tile(y_owner * 2 + dest, 1, tile), y_raw.at[stage, core, rows(tile)], y_sent.at[tile], y_got.at[stage, core, tile], y_chip * 2 + dest).start()
        first = y_chip * 2 + mate_core if stage == 0 else mate
        second = x_chip * 2 + mate_core if stage == 0 else mate
        remote(grad_tile(first, 0, tile), mate_raw.at[2 * stage, rows(tile)], mate_sent.at[tile], mate_got.at[2 * stage, tile], mate).start()
        remote(grad_tile(second, 1, tile), mate_raw.at[2 * stage + 1, rows(tile)], mate_sent.at[tile], mate_got.at[2 * stage + 1, tile], mate).start()

    def arrived(ref, sem):
        remote(ref, ref, sem, sem, mate).wait_recv()

    def wait_raw(stage, tile):
        for source in range(2):
            arrived(x_raw.at[stage, source, rows(tile)], x_got.at[stage, source, tile])
            arrived(y_raw.at[stage, source, rows(tile)], y_got.at[stage, source, tile])
        for part in range(2):
            arrived(mate_raw.at[2 * stage + part, rows(tile)], mate_got.at[2 * stage + part, tile])

    def loads(stage, tile):
        owners = (y_peer, x_peer) if stage == 0 else (me, me)
        out = []
        for part in range(2):
            far = x_raw if part == 0 else y_raw
            sources = [grad_tile(owners[part], part, tile), mate_raw.at[2 * stage + part, rows(tile)], far.at[stage, 0, rows(tile)], far.at[stage, 1, rows(tile)]]
            for k, source in enumerate(sources):
                out.append(pltpu.make_async_copy(source, blocks.at[part, k], load_sem.at[part, k]))
        return out

    @pl.loop(0, tiles)
    def _(tile):
        send_raw(0, tile)

    @pl.loop(0, tiles)
    def _(tile):
        send_raw(1, tile)
        wait_raw(0, tile)
        copies = loads(0, tile)
        for copy in copies:
            copy.start()
        for part in range(2):
            for copy in copies[4 * part:4 * part + 4]:
                copy.wait()

            @pl.loop(0, TILE // SLAB)
            def _(slab):
                at = pl.ds(pl.multiple_of(slab * SLAB, SLAB), SLAB)
                parts = [blocks[part, k, at, :].astype(jnp.float32) for k in range(4)]
                relay[part, tile, at, :] = (parts[0] + parts[1]) + (parts[2] + parts[3])

            if part == 0:
                remote(relay.at[0, tile], y_sum.at[tile], ys_sent.at[tile], ys_got.at[tile], y_peer).start()
            else:
                remote(relay.at[1, tile], x_sum.at[tile], xs_sent.at[tile], xs_got.at[tile], x_peer).start()

    squares[...] = jnp.zeros_like(squares)

    def total_tile(part, tile):
        return total_ref.at[pl.ds(pl.multiple_of(part * half + tile * TILE, TILE), TILE), :]

    @pl.loop(0, tiles)
    def _(tile):
        wait_raw(1, tile)
        copies = loads(1, tile)
        for copy in copies:
            copy.start()
        for part in range(2):
            for copy in copies[4 * part:4 * part + 4]:
                copy.wait()
            if part == 0:
                arrived(y_sum.at[tile], ys_got.at[tile])
            else:
                arrived(x_sum.at[tile], xs_got.at[tile])
            far_sum = (y_sum, x_sum)[part]

            @pl.when(tile > 0)
            def _():
                pltpu.make_async_copy(finals.at[part], total_tile(part, tile), store_sem.at[part]).wait()

            @pl.loop(0, TILE // SLAB)
            def _(slab):
                at = pl.ds(pl.multiple_of(slab * SLAB, SLAB), SLAB)
                parts = [blocks[part, k, at, :].astype(jnp.float32) for k in range(4)]
                mean = ((parts[0] + parts[1]) + (parts[2] + parts[3]) + far_sum[tile, at, :]) * 0.125
                finals[part, at, :] = mean
                squares[...] += jnp.sum((mean * mean).reshape(SLAB // 8, 8, mean.shape[1]), axis=0)

            pltpu.make_async_copy(finals.at[part], total_tile(part, tile), store_sem.at[part]).start()

    width = squares.shape[1]
    packed = squares[:, 0:128]
    for lane in range(1, width // 128):
        packed = packed + squares[:, lane * 128:lane * 128 + 128]
    norm_mine[...] = packed
    norm_all[me] = packed
    for part in range(2):
        pltpu.make_async_copy(finals.at[part], total_tile(part, 0), store_sem.at[part]).wait()
    for k, partner in enumerate(everyone):
        remote(norm_mine, norm_all.at[me], norm_sent.at[k], norm_got.at[me], partner).start()
    for partner in everyone:
        arrived(norm_all.at[partner], norm_got.at[partner])
    squared = norm_all[0]
    for k in range(1, 8):
        squared = squared + norm_all[k]
    norm = jnp.sqrt(jnp.sum(squared))
    clip_ref[...] = jnp.broadcast_to(jnp.minimum(1.0, 1.0 / (norm + 1e-6)), clip_ref.shape)

    for k, partner in enumerate(everyone):
        remote(norm_mine, norm_mine, norm_sent.at[k], norm_sent.at[k], partner).wait_send()

    @pl.loop(0, tiles)
    def _(tile):
        for ref, sem in ((x_raw.at[:, :, rows(tile)], x_sent), (y_raw.at[:, :, rows(tile)], y_sent), (mate_raw.at[:, rows(tile)], mate_sent),
                         (x_sum.at[tile], xs_sent), (y_sum.at[tile], ys_sent)):
            remote(ref, ref, sem.at[tile], sem.at[tile], mate).wait_send()


def reduce_grads(local_grads, shard):
    width = local_grads.shape[2]
    half = shard // 2
    tiles = half // TILE
    any_spec = pl.BlockSpec(memory_space=pl.ANY)
    bf16, f32 = jnp.bfloat16, jnp.float32
    dma = pltpu.SemaphoreType.DMA
    outs = pl.pallas_call(
        functools.partial(reduce_kernel, shard),
        out_shape=[
            jax.ShapeDtypeStruct((shard, width), f32),
            jax.ShapeDtypeStruct((8, 128), f32),
            jax.ShapeDtypeStruct((2, 2, half, width), bf16),
            jax.ShapeDtypeStruct((2, 2, half, width), bf16),
            jax.ShapeDtypeStruct((4, half, width), bf16),
        ],
        in_specs=[any_spec],
        out_specs=[any_spec, pl.BlockSpec(memory_space=pltpu.VMEM)] + [any_spec] * 3,
        scratch_shapes=[
            pltpu.VMEM((2, tiles, TILE, width), f32),
            pltpu.VMEM((2, 4, TILE, width), bf16),
            pltpu.VMEM((tiles, TILE, width), f32),
            pltpu.VMEM((tiles, TILE, width), f32),
            pltpu.VMEM((2, TILE, width), f32),
            pltpu.VMEM((8, width), f32),
            pltpu.VMEM((8, 128), f32),
            pltpu.VMEM((8, 8, 128), f32),
            dma((tiles,)), dma((tiles,)), dma((tiles,)), dma((tiles,)), dma((tiles,)),
            dma((2, 2, tiles)), dma((2, 2, tiles)), dma((4, tiles)), dma((tiles,)), dma((tiles,)),
            dma((2, 4)), dma((2,)), dma((7,)), dma((8,)),
        ],
        compiler_params=pltpu.CompilerParams(collective_id=0, has_side_effects=True, vmem_limit_bytes=56 * 2 ** 20),
        name='reduce_grads',
    )(local_grads)
    return outs[0], outs[1]


def adam_kernel(first_row, shard, total_rows, rate_ref, clip_ref, grad, master, first, second, *refs):
    new_master, new_first, new_second, rounded = refs[-4:]
    width = grad.shape[1]
    run_starts, lr_values, decay_values = layout_runs(width, total_rows)
    start = lax.axis_index('dp') * shard + first_row + pl.program_id(0) * ADAM_TILE
    rate = rate_ref[0]
    clip_scale = clip_ref[0:1, 0:1]

    @pl.loop(0, ADAM_TILE // ADAM_SLAB)
    def _(slab):
        at = pl.ds(pl.multiple_of(slab * ADAM_SLAB, ADAM_SLAB), ADAM_SLAB)
        row = start + slab * ADAM_SLAB + lax.broadcasted_iota(jnp.int32, (ADAM_SLAB, 128), 0)
        lr_factor = jnp.full((ADAM_SLAB, 128), lr_values[0], jnp.float32)
        decay = jnp.full((ADAM_SLAB, 128), decay_values[0], jnp.float32)
        for k in range(1, len(run_starts)):
            later = row >= run_starts[k]
            if lr_values[k] != lr_values[k - 1]:
                lr_factor = jnp.where(later, lr_values[k], lr_factor)
            if decay_values[k] != decay_values[k - 1]:
                decay = jnp.where(later, decay_values[k], decay)
        step_size = rate * lr_factor
        for lane in range(width // 128):
            cols = pl.ds(lane * 128, 128)
            clipped = grad[at, cols] * clip_scale
            old = master[at, cols]
            next_first = 0.9 * first[at, cols] + 0.1 * clipped
            next_second = 0.99 * second[at, cols] + 0.01 * (clipped * clipped)
            first_hat = next_first / (1.0 - 0.9 ** ADAM_STEP)
            second_hat = next_second / (1.0 - 0.99 ** ADAM_STEP)
            value = old - step_size * (first_hat / (jnp.sqrt(second_hat) + 1e-8) + decay * old)
            new_first[at, cols] = next_first
            new_second[at, cols] = next_second
            new_master[at, cols] = value
            rounded[at, cols] = value.astype(jnp.bfloat16)


def adam_chunk(first_row, chunk, rate, clip, grad, states, previous, total_rows):
    shard, width = grad.shape
    block = pl.BlockSpec((ADAM_TILE, width), lambda step: (first_row // ADAM_TILE + step, 0))
    own = pl.BlockSpec((ADAM_TILE, width), lambda step: (step, 0))
    any_spec = pl.BlockSpec(memory_space=pl.ANY)
    smem = pl.BlockSpec(memory_space=pltpu.SMEM)
    vmem = pl.BlockSpec((8, 128), lambda step: (0, 0))
    full = jax.ShapeDtypeStruct((shard, width), jnp.float32)
    return pl.pallas_call(
        functools.partial(adam_kernel, first_row, shard, total_rows),
        grid=(chunk // ADAM_TILE,),
        out_shape=[full] * 3 + [jax.ShapeDtypeStruct((chunk, width), jnp.bfloat16)],
        in_specs=[smem, vmem] + [block] * 4 + [any_spec] * len(previous),
        out_specs=[block] * 3 + [own],
        input_output_aliases={6 + k: k for k in range(len(previous))},
        compiler_params=pltpu.CompilerParams(vmem_limit_bytes=56 * 2 ** 20),
        cost_estimate=pl.CostEstimate(flops=ADAM_FLOPS * chunk * width, bytes_accessed=30 * chunk * width, transcendentals=0),
    )(rate, clip, grad, *states, *previous)


def place_kernel(spots, shard, *refs):
    count = len(spots)
    pieces = refs[:count]
    target, stored = refs[-2:]
    me, core, _, x_chip, y_chip, d_chip = places()
    chips = {'m': me // 2, 'x': x_chip, 'y': y_chip, 'd': d_chip}

    def store(k):
        chip, side, first_row = spots[k]
        owner = chips[chip] * 2 + (core if side == 0 else 1 - core)
        at = pl.multiple_of(owner * shard + first_row, 64)
        return pltpu.make_async_copy(pieces[k], target.at[pl.ds(at, pieces[k].shape[0])], stored.at[k])

    for k in range(count):
        store(k).start()
    for k in range(count):
        store(k).wait()


def place(shard, labelled, target, total_rows):
    spots = [spot for spot, _ in labelled]
    pieces = [piece for _, piece in labelled]
    width = pieces[0].shape[1]
    count = len(pieces)
    any_spec = pl.BlockSpec(memory_space=pl.ANY)
    previous = [] if target is None else [target]
    size = sum(piece.size for piece in pieces)
    return pl.pallas_call(
        functools.partial(place_kernel, spots, shard),
        out_shape=jax.ShapeDtypeStruct((total_rows, width), jnp.bfloat16),
        in_specs=[pl.BlockSpec(memory_space=pltpu.VMEM)] * count + [any_spec] * len(previous),
        out_specs=any_spec,
        scratch_shapes=[pltpu.SemaphoreType.DMA((count,))],
        input_output_aliases={count: 0} if previous else {},
        compiler_params=pltpu.CompilerParams(vmem_limit_bytes=PLACE_VMEM),
        cost_estimate=pl.CostEstimate(flops=PLACE_FLOPS * size, bytes_accessed=4 * size, transcendentals=0),
    )(*pieces, *previous)


def swap(value, bit):
    return lax.ppermute(value, 'dp', [(i, i ^ bit) for i in range(8)])


def solution(mesh):
    dev_count = mesh.shape['dp']

    def device_step(local_grads, master, mom_first, mom_second, learn_rate):
        shard = master.shape[0]
        total_rows = shard * dev_count
        grad_shard, clip = reduce_grads(local_grads, shard)
        rate = learn_rate.reshape(1)
        previous = []
        chunks = []
        first_row = 0
        for chunk in CHUNKS:
            outs = adam_chunk(first_row, chunk, rate, clip, grad_shard, (master, mom_first, mom_second), previous, total_rows)
            previous = list(outs[:3])
            chunks.append((first_row, outs[3]))
            first_row += chunk
        near, far = [], []
        for index, (first_row, mine) in enumerate(chunks):
            from_x = swap(mine, 2)
            from_y = swap(mine, 4)
            from_d = swap(from_x, 4) if index % 2 == 0 else swap(from_y, 2)
            near += [(('m', 0, first_row), mine), (('m', 1, first_row), swap(mine, 1))]
            near += [(('x', 0, first_row), from_x), (('x', 1, first_row), swap(from_x, 1))]
            near += [(('y', 0, first_row), from_y), (('y', 1, first_row), swap(from_y, 1))]
            far += [(('d', 0, first_row), from_d), (('d', 1, first_row), swap(from_d, 1))]
        target = None
        for pair in range(len(CHUNKS) // 2):
            target = place(shard, near[12 * pair:12 * pair + 12], target, total_rows)
        for pair in range(len(CHUNKS) // 2):
            target = place(shard, far[4 * pair:4 * pair + 4], target, total_rows)
        return (*previous, target)

    return jax.shard_map(device_step, mesh=mesh, in_specs=(P('dp', None, None), P('dp', None), P('dp', None), P('dp', None), P()), out_specs=(P('dp', None), P('dp', None), P('dp', None), P(None, None)), check_vma=False)
```

```python
import functools

import jax
import jax.numpy as jnp
from jax import lax
from jax.experimental import pallas as pl
from jax.experimental.pallas import tpu as pltpu
from jax.sharding import PartitionSpec as P

LAYERS = 2
MIX_RANK = 32
DECAY_RANK = 64
ADAM_STEP = 10
MESH = pl.DeviceIdType.MESH
TILE = 384
PIECE = 128
SLAB = 32
ADAM_TILE = 192
ADAM_SLAB = 32
CHUNKS = (384, 384, 1152, 1152, 960, 960, 384, 384, 192, 192)
ADAM_FLOPS = 60
PLACE_FLOPS = 16
PLACE_VMEM = 24 * 2 ** 20


def layout_runs(model_width, total_rows):
    ffn_width = 7 * model_width // 2
    layer_rows = 6 * model_width + 2 * ffn_width + 16 + 10 * MIX_RANK + 2 * DECAY_RANK
    vocab_rows = (total_rows - LAYERS * layer_rows - 4) // 2
    base_rule = (1.0, 0.0)
    decay_rule = (1.0, 0.1)
    time_rule = (2.0, 0.0)
    pieces = [(vocab_rows, decay_rule)]
    for layer_idx in range(LAYERS):
        lead_rows = 12 if layer_idx == 0 else 10
        pieces = pieces + [(lead_rows + 10 * MIX_RANK, base_rule), (1, time_rule), (2 * DECAY_RANK, base_rule), (1, time_rule), (5 * model_width, decay_rule), (4, base_rule), (2 * ffn_width + model_width, decay_rule)]
    pieces = pieces + [(2, base_rule), (vocab_rows, decay_rule)]
    run_starts = []
    next_row = 0
    for run_len, run_rule in pieces:
        run_starts.append(next_row)
        next_row = next_row + run_len
    lr_values = [run_rule[0] for run_len, run_rule in pieces]
    decay_values = [run_rule[1] for run_len, run_rule in pieces]
    return run_starts, lr_values, decay_values


def places():
    me = lax.axis_index('dp')
    core = me % 2
    x = (me // 2) % 2
    y = me // 4
    x_chip = y * 2 + (1 - x)
    y_chip = (1 - y) * 2 + x
    d_chip = (1 - y) * 2 + (1 - x)
    return me, core, me + 1 - 2 * core, x_chip, y_chip, d_chip


def greet(partners):
    barrier = pltpu.get_barrier_semaphore()
    for partner in partners:
        pl.semaphore_signal(barrier, inc=1, device_id=(partner,), device_id_type=MESH)
    pl.semaphore_wait(barrier, len(partners))


def update_slab(row, total_rows, rate, clip_scale, grad, master, first, second, put):
    width = grad.shape[1]
    run_starts, lr_values, decay_values = layout_runs(width, total_rows)
    lr_factor = jnp.full(row.shape, lr_values[0], jnp.float32)
    decay = jnp.full(row.shape, decay_values[0], jnp.float32)
    for k in range(1, len(run_starts)):
        later = row >= run_starts[k]
        if lr_values[k] != lr_values[k - 1]:
            lr_factor = jnp.where(later, lr_values[k], lr_factor)
        if decay_values[k] != decay_values[k - 1]:
            decay = jnp.where(later, decay_values[k], decay)
    step_size = rate * lr_factor
    for lane in range(width // 128):
        cols = pl.ds(lane * 128, 128)
        clipped = grad[:, cols] * clip_scale
        old = master[:, cols]
        next_first = 0.9 * first[:, cols] + 0.1 * clipped
        next_second = 0.99 * second[:, cols] + 0.01 * (clipped * clipped)
        first_hat = next_first / (1.0 - 0.9 ** ADAM_STEP)
        second_hat = next_second / (1.0 - 0.99 ** ADAM_STEP)
        value = old - step_size * (first_hat / (jnp.sqrt(second_hat) + 1e-8) + decay * old)
        put(cols, value, next_first, next_second)


def adam_kernel(first_row, shard, total_rows, rate_ref, clip_ref, grad, master, first, second, *refs):
    new_master, new_first, new_second, rounded = refs[-4:]
    start = lax.axis_index('dp') * shard + first_row + pl.program_id(0) * ADAM_TILE
    rate = rate_ref[0]
    clip_scale = clip_ref[0:1, 0:1]

    @pl.loop(0, ADAM_TILE // ADAM_SLAB)
    def _(slab):
        at = pl.ds(pl.multiple_of(slab * ADAM_SLAB, ADAM_SLAB), ADAM_SLAB)
        row = start + slab * ADAM_SLAB + lax.broadcasted_iota(jnp.int32, (ADAM_SLAB, 128), 0)

        def put(cols, value, next_first, next_second):
            new_first[at, cols] = next_first
            new_second[at, cols] = next_second
            new_master[at, cols] = value
            rounded[at, cols] = value.astype(jnp.bfloat16)

        update_slab(row, total_rows, rate, clip_scale, grad.at[at], master.at[at], first.at[at], second.at[at], put)


def reduce_kernel(shard, rate_in, grads, master, first, second, total_ref, clip_out, rounded_ref, x_raw, y_raw, mate_raw,
                  relay, blocks, x_sum, y_sum, finals, head_grad, head_state, head_rounded, head_sem, rate_ref, clip_ref, squares, norm_mine, norm_all,
                  x_sent, y_sent, mate_sent, xs_sent, ys_sent, x_got, y_got, mate_got, xs_got, ys_got,
                  load_sem, store_sem, norm_sent, norm_got):
    half = shard // 2
    tiles = half // TILE
    me, core, mate, x_chip, y_chip, d_chip = places()
    mate_core = 1 - core
    x_peer, y_peer = x_chip * 2 + core, y_chip * 2 + core
    everyone = [mate, x_chip * 2, x_chip * 2 + 1, y_chip * 2, y_chip * 2 + 1, d_chip * 2, d_chip * 2 + 1]
    greet(everyone)
    head = [pltpu.make_async_copy(state.at[pl.ds(0, TILE)], head_state.at[k], head_sem.at[k]) for k, state in enumerate((master, first, second))]
    head.append(pltpu.make_async_copy(rate_in, rate_ref, head_sem.at[3]))

    def rows(tile):
        return pl.ds(pl.multiple_of(tile * TILE, TILE), TILE)

    def grad_tile(owner, part, tile):
        return grads.at[0, pl.ds(pl.multiple_of(owner * shard + part * half + tile * TILE, TILE), TILE), :]

    def remote(src, dst, sent, got, device):
        return pltpu.make_async_remote_copy(src_ref=src, dst_ref=dst, send_sem=sent, recv_sem=got, device_id=(device,), device_id_type=MESH)

    def send_raw(stage, tile):
        x_owner = d_chip if stage == 0 else x_chip
        y_owner = d_chip if stage == 0 else y_chip
        for dest in range(2):
            remote(grad_tile(x_owner * 2 + dest, 0, tile), x_raw.at[stage, core, rows(tile)], x_sent.at[tile], x_got.at[stage, core, tile], x_chip * 2 + dest).start()
            remote(grad_tile(y_owner * 2 + dest, 1, tile), y_raw.at[stage, core, rows(tile)], y_sent.at[tile], y_got.at[stage, core, tile], y_chip * 2 + dest).start()
        first = y_chip * 2 + mate_core if stage == 0 else mate
        second = x_chip * 2 + mate_core if stage == 0 else mate
        remote(grad_tile(first, 0, tile), mate_raw.at[2 * stage, rows(tile)], mate_sent.at[tile], mate_got.at[2 * stage, tile], mate).start()
        remote(grad_tile(second, 1, tile), mate_raw.at[2 * stage + 1, rows(tile)], mate_sent.at[tile], mate_got.at[2 * stage + 1, tile], mate).start()

    def arrived(ref, sem):
        remote(ref, ref, sem, sem, mate).wait_recv()

    def wait_raw(stage, tile):
        for source in range(2):
            arrived(x_raw.at[stage, source, rows(tile)], x_got.at[stage, source, tile])
            arrived(y_raw.at[stage, source, rows(tile)], y_got.at[stage, source, tile])
        for part in range(2):
            arrived(mate_raw.at[2 * stage + part, rows(tile)], mate_got.at[2 * stage + part, tile])

    def loads(stage, tile):
        owners = (y_peer, x_peer) if stage == 0 else (me, me)
        out = []
        for part in range(2):
            far = x_raw if part == 0 else y_raw
            sources = [grad_tile(owners[part], part, tile), mate_raw.at[2 * stage + part, rows(tile)], far.at[stage, 0, rows(tile)], far.at[stage, 1, rows(tile)]]
            for k, source in enumerate(sources):
                out.append(pltpu.make_async_copy(source, blocks.at[part, k], load_sem.at[part, k]))
        return out

    @pl.loop(0, tiles)
    def _(tile):
        send_raw(0, tile)

    @pl.loop(0, tiles)
    def _(tile):
        send_raw(1, tile)
        wait_raw(0, tile)
        copies = loads(0, tile)
        for copy in copies:
            copy.start()
        for part in range(2):
            for copy in copies[4 * part:4 * part + 4]:
                copy.wait()

            for piece in range(TILE // PIECE):
                here = pl.ds(piece * PIECE, PIECE)

                @pl.loop(piece * PIECE // SLAB, (piece + 1) * PIECE // SLAB)
                def _(slab):
                    at = pl.ds(pl.multiple_of(slab * SLAB, SLAB), SLAB)
                    parts = [blocks[part, k, at, :].astype(jnp.float32) for k in range(4)]
                    relay[part, tile, at, :] = (parts[0] + parts[1]) + (parts[2] + parts[3])

                if part == 0:
                    remote(relay.at[0, tile, here], y_sum.at[tile, here], ys_sent.at[tile], ys_got.at[tile, piece], y_peer).start()
                else:
                    remote(relay.at[1, tile, here], x_sum.at[tile, here], xs_sent.at[tile], xs_got.at[tile, piece], x_peer).start()

    for copy in head:
        copy.start()
    squares[...] = jnp.zeros_like(squares)

    def total_tile(part, tile):
        return total_ref.at[pl.ds(pl.multiple_of(part * half + tile * TILE, TILE), TILE), :]

    @pl.loop(0, tiles)
    def _(tile):
        wait_raw(1, tile)
        copies = loads(1, tile)
        for copy in copies:
            copy.start()
        for part in range(2):
            for copy in copies[4 * part:4 * part + 4]:
                copy.wait()
            far_sum, far_got = (y_sum, x_sum)[part], (ys_got, xs_got)[part]

            @pl.when(tile > 0)
            def _():
                pltpu.make_async_copy(finals.at[part], total_tile(part, tile), store_sem.at[part]).wait()

            for piece in range(TILE // PIECE):
                arrived(far_sum.at[tile, pl.ds(piece * PIECE, PIECE)], far_got.at[tile, piece])

                @pl.loop(piece * PIECE // SLAB, (piece + 1) * PIECE // SLAB)
                def _(slab):
                    at = pl.ds(pl.multiple_of(slab * SLAB, SLAB), SLAB)
                    parts = [blocks[part, k, at, :].astype(jnp.float32) for k in range(4)]
                    mean = ((parts[0] + parts[1]) + (parts[2] + parts[3]) + far_sum[tile, at, :]) * 0.125
                    finals[part, at, :] = mean
                    if part == 0:
                        @pl.when(tile == 0)
                        def _():
                            head_grad[at, :] = mean
                    squares[...] += jnp.sum((mean * mean).reshape(SLAB // 8, 8, mean.shape[1]), axis=0)

            pltpu.make_async_copy(finals.at[part], total_tile(part, tile), store_sem.at[part]).start()

    width = squares.shape[1]
    packed = squares[:, 0:128]
    for lane in range(1, width // 128):
        packed = packed + squares[:, lane * 128:lane * 128 + 128]
    norm_mine[...] = packed
    norm_all[me] = packed
    for k, partner in enumerate(everyone):
        remote(norm_mine, norm_all.at[me], norm_sent.at[k], norm_got.at[me], partner).start()
    for part in range(2):
        pltpu.make_async_copy(finals.at[part], total_tile(part, 0), store_sem.at[part]).wait()
    for copy in head:
        copy.wait()
    for partner in everyone:
        arrived(norm_all.at[partner], norm_got.at[partner])
    squared = norm_all[0]
    for k in range(1, 8):
        squared = squared + norm_all[k]
    norm = jnp.sqrt(jnp.sum(squared, keepdims=True))
    clip_scale = jnp.minimum(1.0, 1.0 / (norm + 1e-6))
    clip_ref[...] = jnp.broadcast_to(clip_scale, clip_ref.shape)
    clip_copy = pltpu.make_async_copy(clip_ref, clip_out, head_sem.at[4])

    def head_slab(slab):
        at = pl.ds(pl.multiple_of(slab * ADAM_SLAB, ADAM_SLAB), ADAM_SLAB)
        row = me * shard + slab * ADAM_SLAB + lax.broadcasted_iota(jnp.int32, (ADAM_SLAB, 128), 0)

        def put(cols, value, next_first, next_second):
            head_rounded[at, cols] = value.astype(jnp.bfloat16)

        update_slab(row, 8 * shard, rate_ref[0], clip_ref[0:1, 0:1], head_grad.at[at], head_state.at[0, at], head_state.at[1, at], head_state.at[2, at], put)

    for piece in range(TILE // PIECE):
        pl.loop(piece * PIECE // ADAM_SLAB, (piece + 1) * PIECE // ADAM_SLAB)(head_slab)
        if piece == 0:
            clip_copy.start()
        here = pl.ds(piece * PIECE, PIECE)
        pltpu.make_async_copy(head_rounded.at[here], rounded_ref.at[here], head_sem.at[5 + piece]).start()

    for k, partner in enumerate(everyone):
        remote(norm_mine, norm_mine, norm_sent.at[k], norm_sent.at[k], partner).wait_send()

    @pl.loop(0, tiles)
    def _(tile):
        for ref, sem in ((x_raw.at[:, :, rows(tile)], x_sent), (y_raw.at[:, :, rows(tile)], y_sent), (mate_raw.at[:, rows(tile)], mate_sent),
                         (x_sum.at[tile], xs_sent), (y_sum.at[tile], ys_sent)):
            remote(ref, ref, sem.at[tile], sem.at[tile], mate).wait_send()

    clip_copy.wait()
    for piece in range(TILE // PIECE):
        here = pl.ds(piece * PIECE, PIECE)
        pltpu.make_async_copy(head_rounded.at[here], rounded_ref.at[here], head_sem.at[5 + piece]).wait()


def reduce_grads(rate, local_grads, master, first, second):
    shard = master.shape[0]
    width = local_grads.shape[2]
    half = shard // 2
    tiles = half // TILE
    any_spec = pl.BlockSpec(memory_space=pl.ANY)
    bf16, f32 = jnp.bfloat16, jnp.float32
    dma = pltpu.SemaphoreType.DMA
    outs = pl.pallas_call(
        functools.partial(reduce_kernel, shard),
        out_shape=[
            jax.ShapeDtypeStruct((shard, width), f32),
            jax.ShapeDtypeStruct((8, 128), f32),
            jax.ShapeDtypeStruct((TILE, width), bf16),
            jax.ShapeDtypeStruct((2, 2, half, width), bf16),
            jax.ShapeDtypeStruct((2, 2, half, width), bf16),
            jax.ShapeDtypeStruct((4, half, width), bf16),
        ],
        in_specs=[any_spec] * 5,
        out_specs=[any_spec] * 6,
        scratch_shapes=[
            pltpu.VMEM((2, tiles, TILE, width), f32),
            pltpu.VMEM((2, 4, TILE, width), bf16),
            pltpu.VMEM((tiles, TILE, width), f32),
            pltpu.VMEM((tiles, TILE, width), f32),
            pltpu.VMEM((2, TILE, width), f32),
            pltpu.VMEM((TILE, width), f32),
            pltpu.VMEM((3, TILE, width), f32),
            pltpu.VMEM((TILE, width), bf16),
            dma((5 + TILE // PIECE,)),
            pltpu.SMEM((1,), f32),
            pltpu.VMEM((8, 128), f32),
            pltpu.VMEM((8, width), f32),
            pltpu.VMEM((8, 128), f32),
            pltpu.VMEM((8, 8, 128), f32),
            dma((tiles,)), dma((tiles,)), dma((tiles,)), dma((tiles,)), dma((tiles,)),
            dma((2, 2, tiles)), dma((2, 2, tiles)), dma((4, tiles)), dma((tiles, TILE // PIECE)), dma((tiles, TILE // PIECE)),
            dma((2, 4)), dma((2,)), dma((7,)), dma((8,)),
        ],
        compiler_params=pltpu.CompilerParams(collective_id=0, has_side_effects=True, vmem_limit_bytes=56 * 2 ** 20),
        name='reduce_grads',
    )(rate, local_grads, master, first, second)
    return outs[:3]


def adam_chunk(first_row, chunk, rate, clip, grad, states, previous, total_rows):
    shard, width = grad.shape
    block = pl.BlockSpec((ADAM_TILE, width), lambda step: (first_row // ADAM_TILE + step, 0))
    own = pl.BlockSpec((ADAM_TILE, width), lambda step: (step, 0))
    any_spec = pl.BlockSpec(memory_space=pl.ANY)
    smem = pl.BlockSpec(memory_space=pltpu.SMEM)
    vmem = pl.BlockSpec((8, 128), lambda step: (0, 0))
    full = jax.ShapeDtypeStruct((shard, width), jnp.float32)
    return pl.pallas_call(
        functools.partial(adam_kernel, first_row, shard, total_rows),
        grid=(chunk // ADAM_TILE,),
        out_shape=[full] * 3 + [jax.ShapeDtypeStruct((chunk, width), jnp.bfloat16)],
        in_specs=[smem, vmem] + [block] * 4 + [any_spec] * len(previous),
        out_specs=[block] * 3 + [own],
        input_output_aliases={6 + k: k for k in range(len(previous))},
        compiler_params=pltpu.CompilerParams(vmem_limit_bytes=56 * 2 ** 20),
        cost_estimate=pl.CostEstimate(flops=ADAM_FLOPS * chunk * width, bytes_accessed=30 * chunk * width, transcendentals=0),
    )(rate, clip, grad, *states, *previous)


def place_kernel(spots, shard, *refs):
    count = len(spots)
    pieces = refs[:count]
    target, stored = refs[-2:]
    me, core, _, x_chip, y_chip, d_chip = places()
    chips = {'m': me // 2, 'x': x_chip, 'y': y_chip, 'd': d_chip}

    def store(k):
        chip, side, first_row = spots[k]
        owner = chips[chip] * 2 + (core if side == 0 else 1 - core)
        at = pl.multiple_of(owner * shard + first_row, 64)
        return pltpu.make_async_copy(pieces[k], target.at[pl.ds(at, pieces[k].shape[0])], stored.at[k])

    for k in range(count):
        store(k).start()
    for k in range(count):
        store(k).wait()


def place(shard, labelled, target, total_rows):
    spots = [spot for spot, _ in labelled]
    pieces = [piece for _, piece in labelled]
    width = pieces[0].shape[1]
    count = len(pieces)
    any_spec = pl.BlockSpec(memory_space=pl.ANY)
    previous = [] if target is None else [target]
    size = sum(piece.size for piece in pieces)
    return pl.pallas_call(
        functools.partial(place_kernel, spots, shard),
        out_shape=jax.ShapeDtypeStruct((total_rows, width), jnp.bfloat16),
        in_specs=[pl.BlockSpec(memory_space=pltpu.VMEM)] * count + [any_spec] * len(previous),
        out_specs=any_spec,
        scratch_shapes=[pltpu.SemaphoreType.DMA((count,))],
        input_output_aliases={count: 0} if previous else {},
        compiler_params=pltpu.CompilerParams(vmem_limit_bytes=PLACE_VMEM),
        cost_estimate=pl.CostEstimate(flops=PLACE_FLOPS * size, bytes_accessed=4 * size, transcendentals=0),
    )(*pieces, *previous)


def swap(value, bit):
    return lax.ppermute(value, 'dp', [(i, i ^ bit) for i in range(8)])


def solution(mesh):
    dev_count = mesh.shape['dp']

    def device_step(local_grads, master, mom_first, mom_second, learn_rate):
        shard = master.shape[0]
        total_rows = shard * dev_count
        rate = learn_rate.reshape(1)
        grad_shard, clip, head_rounded = reduce_grads(rate, local_grads, master, mom_first, mom_second)
        previous = []
        chunks = []
        for index in (*range(1, len(CHUNKS)), 0):
            first_row = sum(CHUNKS[:index])
            outs = adam_chunk(first_row, CHUNKS[index], rate, clip, grad_shard, (master, mom_first, mom_second), previous, total_rows)
            previous = list(outs[:3])
            chunks.append((first_row, outs[3]))
        chunks = [(0, head_rounded)] + chunks[:-1]
        near, far = [], []
        for index, (first_row, mine) in enumerate(chunks):
            from_x = swap(mine, 2)
            from_y = swap(mine, 4)
            from_d = swap(from_x, 4) if index % 2 == 0 else swap(from_y, 2)
            near += [(('m', 0, first_row), mine), (('m', 1, first_row), swap(mine, 1))]
            near += [(('x', 0, first_row), from_x), (('x', 1, first_row), swap(from_x, 1))]
            near += [(('y', 0, first_row), from_y), (('y', 1, first_row), swap(from_y, 1))]
            far += [(('d', 0, first_row), from_d), (('d', 1, first_row), swap(from_d, 1))]
        target = None
        for pair in range(len(CHUNKS) // 2):
            target = place(shard, near[12 * pair:12 * pair + 12], target, total_rows)
        for pair in range(len(CHUNKS) // 2):
            target = place(shard, far[4 * pair:4 * pair + 4], target, total_rows)
        return (*previous, target)

    return jax.shard_map(device_step, mesh=mesh, in_specs=(P('dp', None, None), P('dp', None), P('dp', None), P('dp', None), P()), out_specs=(P('dp', None), P('dp', None), P('dp', None), P(None, None)), check_vma=False)
```

```python
import functools

import jax
import jax.numpy as jnp
from jax import lax
from jax.experimental import pallas as pl
from jax.experimental.pallas import tpu as pltpu
from jax.sharding import PartitionSpec as P

LAYERS = 2
MIX_RANK = 32
DECAY_RANK = 64
ADAM_STEP = 10
MESH = pl.DeviceIdType.MESH
RAW = 1536
TILE = 384
PIECE = 128
SLAB = 32
ADAM_TILE = 192
ADAM_SLAB = 32
CHUNKS = (384, 384, 1152, 1152, 960, 960, 384, 384, 192, 192)
ADAM_FLOPS = 60
PLACE_FLOPS = 16
PLACE_VMEM = 24 * 2 ** 20


def layout_runs(model_width, total_rows):
    ffn_width = 7 * model_width // 2
    layer_rows = 6 * model_width + 2 * ffn_width + 16 + 10 * MIX_RANK + 2 * DECAY_RANK
    vocab_rows = (total_rows - LAYERS * layer_rows - 4) // 2
    base_rule = (1.0, 0.0)
    decay_rule = (1.0, 0.1)
    time_rule = (2.0, 0.0)
    pieces = [(vocab_rows, decay_rule)]
    for layer_idx in range(LAYERS):
        lead_rows = 12 if layer_idx == 0 else 10
        pieces = pieces + [(lead_rows + 10 * MIX_RANK, base_rule), (1, time_rule), (2 * DECAY_RANK, base_rule), (1, time_rule), (5 * model_width, decay_rule), (4, base_rule), (2 * ffn_width + model_width, decay_rule)]
    pieces = pieces + [(2, base_rule), (vocab_rows, decay_rule)]
    run_starts = []
    next_row = 0
    for run_len, run_rule in pieces:
        run_starts.append(next_row)
        next_row = next_row + run_len
    lr_values = [run_rule[0] for run_len, run_rule in pieces]
    decay_values = [run_rule[1] for run_len, run_rule in pieces]
    return run_starts, lr_values, decay_values


def places():
    me = lax.axis_index('dp')
    core = me % 2
    x = (me // 2) % 2
    y = me // 4
    x_chip = y * 2 + (1 - x)
    y_chip = (1 - y) * 2 + x
    d_chip = (1 - y) * 2 + (1 - x)
    return me, core, me + 1 - 2 * core, x_chip, y_chip, d_chip


def greet(partners):
    barrier = pltpu.get_barrier_semaphore()
    for partner in partners:
        pl.semaphore_signal(barrier, inc=1, device_id=(partner,), device_id_type=MESH)
    pl.semaphore_wait(barrier, len(partners))


def update_slab(row, total_rows, rate, clip_scale, grad, master, first, second, put):
    width = grad.shape[1]
    run_starts, lr_values, decay_values = layout_runs(width, total_rows)
    lr_factor = jnp.full(row.shape, lr_values[0], jnp.float32)
    decay = jnp.full(row.shape, decay_values[0], jnp.float32)
    for k in range(1, len(run_starts)):
        later = row >= run_starts[k]
        if lr_values[k] != lr_values[k - 1]:
            lr_factor = jnp.where(later, lr_values[k], lr_factor)
        if decay_values[k] != decay_values[k - 1]:
            decay = jnp.where(later, decay_values[k], decay)
    step_size = rate * lr_factor
    for lane in range(width // 128):
        cols = pl.ds(lane * 128, 128)
        clipped = grad[:, cols] * clip_scale
        old = master[:, cols]
        next_first = 0.9 * first[:, cols] + 0.1 * clipped
        next_second = 0.99 * second[:, cols] + 0.01 * (clipped * clipped)
        first_hat = next_first * (1.0 / (1.0 - 0.9 ** ADAM_STEP))
        second_hat = next_second * (1.0 / (1.0 - 0.99 ** ADAM_STEP))
        value = old - step_size * (first_hat / (jnp.sqrt(second_hat) + 1e-8) + decay * old)
        put(cols, value, next_first, next_second)


def adam_kernel(first_row, shard, total_rows, rate_ref, clip_ref, grad, master, first, second, *refs):
    new_master, new_first, new_second, rounded = refs[-4:]
    start = lax.axis_index('dp') * shard + first_row + pl.program_id(0) * ADAM_TILE
    rate = rate_ref[0]
    clip_scale = clip_ref[0:1, 0:1]

    @pl.loop(0, ADAM_TILE // ADAM_SLAB)
    def _(slab):
        at = pl.ds(pl.multiple_of(slab * ADAM_SLAB, ADAM_SLAB), ADAM_SLAB)
        row = start + slab * ADAM_SLAB + lax.broadcasted_iota(jnp.int32, (ADAM_SLAB, 128), 0)

        def put(cols, value, next_first, next_second):
            new_first[at, cols] = next_first
            new_second[at, cols] = next_second
            new_master[at, cols] = value
            rounded[at, cols] = value.astype(jnp.bfloat16)

        update_slab(row, total_rows, rate, clip_scale, grad.at[at], master.at[at], first.at[at], second.at[at], put)


def reduce_kernel(shard, rate_in, grads, master, first, second, total_ref, clip_out, rounded_ref, x_raw, y_raw, mate_raw,
                  relay, blocks, x_sum, y_sum, finals, head_grad, head_state, head_rounded, head_sem, rate_ref, clip_ref, squares, norm_mine, norm_all,
                  x_sent, y_sent, mate_sent, xs_sent, ys_sent, x_got, y_got, mate_got, xs_got, ys_got,
                  load_sem, store_sem, norm_sent, norm_got):
    half = shard // 2
    tiles = half // TILE
    me, core, mate, x_chip, y_chip, d_chip = places()
    mate_core = 1 - core
    x_peer, y_peer = x_chip * 2 + core, y_chip * 2 + core
    everyone = [mate, x_chip * 2, x_chip * 2 + 1, y_chip * 2, y_chip * 2 + 1, d_chip * 2, d_chip * 2 + 1]
    greet(everyone)
    head = [pltpu.make_async_copy(state.at[pl.ds(0, TILE)], head_state.at[k], head_sem.at[k]) for k, state in enumerate((master, first, second))]
    head.append(pltpu.make_async_copy(rate_in, rate_ref, head_sem.at[3]))

    def rows(tile):
        return pl.ds(pl.multiple_of(tile * TILE, TILE), TILE)

    def grad_tile(owner, part, tile):
        return grads.at[0, pl.ds(pl.multiple_of(owner * shard + part * half + tile * TILE, TILE), TILE), :]

    def remote(src, dst, sent, got, device):
        return pltpu.make_async_remote_copy(src_ref=src, dst_ref=dst, send_sem=sent, recv_sem=got, device_id=(device,), device_id_type=MESH)

    def raw_rows(block):
        return pl.ds(pl.multiple_of(block * RAW, RAW), RAW)

    def grad_block(owner, part, block):
        return grads.at[0, pl.ds(pl.multiple_of(owner * shard + part * half + block * RAW, TILE), RAW), :]

    def send_raw(stage, block):
        x_owner = d_chip if stage == 0 else x_chip
        y_owner = d_chip if stage == 0 else y_chip
        for dest in range(2):
            remote(grad_block(x_owner * 2 + dest, 0, block), x_raw.at[stage, core, raw_rows(block)], x_sent.at[block], x_got.at[stage, core, block], x_chip * 2 + dest).start()
            remote(grad_block(y_owner * 2 + dest, 1, block), y_raw.at[stage, core, raw_rows(block)], y_sent.at[block], y_got.at[stage, core, block], y_chip * 2 + dest).start()
        first = y_chip * 2 + mate_core if stage == 0 else mate
        second = x_chip * 2 + mate_core if stage == 0 else mate
        remote(grad_block(first, 0, block), mate_raw.at[2 * stage, raw_rows(block)], mate_sent.at[block], mate_got.at[2 * stage, block], mate).start()
        remote(grad_block(second, 1, block), mate_raw.at[2 * stage + 1, raw_rows(block)], mate_sent.at[block], mate_got.at[2 * stage + 1, block], mate).start()

    def arrived(ref, sem):
        remote(ref, ref, sem, sem, mate).wait_recv()

    def wait_raw(stage, tile):
        @pl.when(tile % (RAW // TILE) == 0)
        def _():
            block = tile // (RAW // TILE)
            for source in range(2):
                arrived(x_raw.at[stage, source, raw_rows(block)], x_got.at[stage, source, block])
                arrived(y_raw.at[stage, source, raw_rows(block)], y_got.at[stage, source, block])
            for part in range(2):
                arrived(mate_raw.at[2 * stage + part, raw_rows(block)], mate_got.at[2 * stage + part, block])

    def loads(stage, tile):
        owners = (y_peer, x_peer) if stage == 0 else (me, me)
        out = []
        for part in range(2):
            far = x_raw if part == 0 else y_raw
            sources = [grad_tile(owners[part], part, tile), mate_raw.at[2 * stage + part, rows(tile)], far.at[stage, 0, rows(tile)], far.at[stage, 1, rows(tile)]]
            for k, source in enumerate(sources):
                out.append(pltpu.make_async_copy(source, blocks.at[part, k], load_sem.at[part, k]))
        return out

    @pl.loop(0, half // RAW)
    def _(block):
        send_raw(0, block)

    @pl.loop(0, tiles)
    def _(tile):
        @pl.when(tile % (RAW // TILE) == 0)
        def _():
            send_raw(1, tile // (RAW // TILE))

        wait_raw(0, tile)
        copies = loads(0, tile)
        for copy in copies:
            copy.start()
        for copy in copies:
            copy.wait()
        for piece in range(TILE // PIECE):
            here = pl.ds(piece * PIECE, PIECE)
            for part in range(2):
                @pl.loop(piece * PIECE // SLAB, (piece + 1) * PIECE // SLAB)
                def _(slab):
                    at = pl.ds(pl.multiple_of(slab * SLAB, SLAB), SLAB)
                    parts = [blocks[part, k, at, :].astype(jnp.float32) for k in range(4)]
                    relay[part, tile, at, :] = (parts[0] + parts[1]) + (parts[2] + parts[3])

                if part == 0:
                    remote(relay.at[0, tile, here], y_sum.at[tile, here], ys_sent.at[tile], ys_got.at[tile, piece], y_peer).start()
                else:
                    remote(relay.at[1, tile, here], x_sum.at[tile, here], xs_sent.at[tile], xs_got.at[tile, piece], x_peer).start()

    for copy in head:
        copy.start()
    squares[...] = jnp.zeros_like(squares)

    def total_tile(part, tile):
        return total_ref.at[pl.ds(pl.multiple_of(part * half + tile * TILE, TILE), TILE), :]

    @pl.loop(0, tiles)
    def _(tile):
        wait_raw(1, tile)
        copies = loads(1, tile)
        for copy in copies:
            copy.start()
        for copy in copies:
            copy.wait()

        @pl.when(tile > 0)
        def _():
            for part in range(2):
                pltpu.make_async_copy(finals.at[part], total_tile(part, tile), store_sem.at[part]).wait()

        for piece in range(TILE // PIECE):
            for part in range(2):
                far_sum, far_got = (y_sum, x_sum)[part], (ys_got, xs_got)[part]
                arrived(far_sum.at[tile, pl.ds(piece * PIECE, PIECE)], far_got.at[tile, piece])

                @pl.loop(piece * PIECE // SLAB, (piece + 1) * PIECE // SLAB)
                def _(slab):
                    at = pl.ds(pl.multiple_of(slab * SLAB, SLAB), SLAB)
                    parts = [blocks[part, k, at, :].astype(jnp.float32) for k in range(4)]
                    mean = ((parts[0] + parts[1]) + (parts[2] + parts[3]) + far_sum[tile, at, :]) * 0.125
                    finals[part, at, :] = mean
                    if part == 0:
                        @pl.when(tile == 0)
                        def _():
                            head_grad[at, :] = mean
                    squares[...] += jnp.sum((mean * mean).reshape(SLAB // 8, 8, mean.shape[1]), axis=0)

        for part in range(2):
            pltpu.make_async_copy(finals.at[part], total_tile(part, tile), store_sem.at[part]).start()

    width = squares.shape[1]
    packed = squares[:, 0:128]
    for lane in range(1, width // 128):
        packed = packed + squares[:, lane * 128:lane * 128 + 128]
    norm_mine[...] = packed
    norm_all[me] = packed
    for k, partner in enumerate(everyone):
        remote(norm_mine, norm_all.at[me], norm_sent.at[k], norm_got.at[me], partner).start()
    for part in range(2):
        pltpu.make_async_copy(finals.at[part], total_tile(part, 0), store_sem.at[part]).wait()
    for copy in head:
        copy.wait()
    for partner in everyone:
        arrived(norm_all.at[partner], norm_got.at[partner])
    squared = norm_all[0]
    for k in range(1, 8):
        squared = squared + norm_all[k]
    norm = jnp.sqrt(jnp.sum(squared, keepdims=True))
    clip_scale = jnp.minimum(1.0, 1.0 / (norm + 1e-6))
    clip_ref[...] = jnp.broadcast_to(clip_scale, clip_ref.shape)
    clip_copy = pltpu.make_async_copy(clip_ref, clip_out, head_sem.at[4])

    def head_slab(slab):
        at = pl.ds(pl.multiple_of(slab * ADAM_SLAB, ADAM_SLAB), ADAM_SLAB)
        row = me * shard + slab * ADAM_SLAB + lax.broadcasted_iota(jnp.int32, (ADAM_SLAB, 128), 0)

        def put(cols, value, next_first, next_second):
            head_rounded[at, cols] = value.astype(jnp.bfloat16)

        update_slab(row, 8 * shard, rate_ref[0], clip_ref[0:1, 0:1], head_grad.at[at], head_state.at[0, at], head_state.at[1, at], head_state.at[2, at], put)

    for piece in range(TILE // PIECE):
        pl.loop(piece * PIECE // ADAM_SLAB, (piece + 1) * PIECE // ADAM_SLAB)(head_slab)
        if piece == 0:
            clip_copy.start()
        here = pl.ds(piece * PIECE, PIECE)
        pltpu.make_async_copy(head_rounded.at[here], rounded_ref.at[here], head_sem.at[5 + piece]).start()

    for k, partner in enumerate(everyone):
        remote(norm_mine, norm_mine, norm_sent.at[k], norm_sent.at[k], partner).wait_send()

    @pl.loop(0, half // RAW)
    def _(block):
        for ref, sem in ((x_raw.at[:, :, raw_rows(block)], x_sent), (y_raw.at[:, :, raw_rows(block)], y_sent), (mate_raw.at[:, raw_rows(block)], mate_sent)):
            remote(ref, ref, sem.at[block], sem.at[block], mate).wait_send()

    @pl.loop(0, tiles)
    def _(tile):
        for ref, sem in ((x_sum.at[tile], xs_sent), (y_sum.at[tile], ys_sent)):
            remote(ref, ref, sem.at[tile], sem.at[tile], mate).wait_send()

    clip_copy.wait()
    for piece in range(TILE // PIECE):
        here = pl.ds(piece * PIECE, PIECE)
        pltpu.make_async_copy(head_rounded.at[here], rounded_ref.at[here], head_sem.at[5 + piece]).wait()


def reduce_grads(rate, local_grads, master, first, second):
    shard = master.shape[0]
    width = local_grads.shape[2]
    half = shard // 2
    tiles = half // TILE
    blocks = half // RAW
    any_spec = pl.BlockSpec(memory_space=pl.ANY)
    bf16, f32 = jnp.bfloat16, jnp.float32
    dma = pltpu.SemaphoreType.DMA
    outs = pl.pallas_call(
        functools.partial(reduce_kernel, shard),
        out_shape=[
            jax.ShapeDtypeStruct((shard, width), f32),
            jax.ShapeDtypeStruct((8, 128), f32),
            jax.ShapeDtypeStruct((TILE, width), bf16),
            jax.ShapeDtypeStruct((2, 2, half, width), bf16),
            jax.ShapeDtypeStruct((2, 2, half, width), bf16),
            jax.ShapeDtypeStruct((4, half, width), bf16),
        ],
        in_specs=[any_spec] * 5,
        out_specs=[any_spec] * 6,
        scratch_shapes=[
            pltpu.VMEM((2, tiles, TILE, width), f32),
            pltpu.VMEM((2, 4, TILE, width), bf16),
            pltpu.VMEM((tiles, TILE, width), f32),
            pltpu.VMEM((tiles, TILE, width), f32),
            pltpu.VMEM((2, TILE, width), f32),
            pltpu.VMEM((TILE, width), f32),
            pltpu.VMEM((3, TILE, width), f32),
            pltpu.VMEM((TILE, width), bf16),
            dma((5 + TILE // PIECE,)),
            pltpu.SMEM((1,), f32),
            pltpu.VMEM((8, 128), f32),
            pltpu.VMEM((8, width), f32),
            pltpu.VMEM((8, 128), f32),
            pltpu.VMEM((8, 8, 128), f32),
            dma((blocks,)), dma((blocks,)), dma((blocks,)), dma((tiles,)), dma((tiles,)),
            dma((2, 2, blocks)), dma((2, 2, blocks)), dma((4, blocks)), dma((tiles, TILE // PIECE)), dma((tiles, TILE // PIECE)),
            dma((2, 4)), dma((2,)), dma((7,)), dma((8,)),
        ],
        compiler_params=pltpu.CompilerParams(collective_id=0, has_side_effects=True, vmem_limit_bytes=56 * 2 ** 20),
        name='reduce_grads',
    )(rate, local_grads, master, first, second)
    return outs[:3]


def adam_chunk(first_row, chunk, rate, clip, grad, states, previous, total_rows):
    shard, width = grad.shape
    block = pl.BlockSpec((ADAM_TILE, width), lambda step: (first_row // ADAM_TILE + step, 0))
    own = pl.BlockSpec((ADAM_TILE, width), lambda step: (step, 0))
    any_spec = pl.BlockSpec(memory_space=pl.ANY)
    smem = pl.BlockSpec(memory_space=pltpu.SMEM)
    vmem = pl.BlockSpec((8, 128), lambda step: (0, 0))
    full = jax.ShapeDtypeStruct((shard, width), jnp.float32)
    return pl.pallas_call(
        functools.partial(adam_kernel, first_row, shard, total_rows),
        grid=(chunk // ADAM_TILE,),
        out_shape=[full] * 3 + [jax.ShapeDtypeStruct((chunk, width), jnp.bfloat16)],
        in_specs=[smem, vmem] + [block] * 4 + [any_spec] * len(previous),
        out_specs=[block] * 3 + [own],
        input_output_aliases={6 + k: k for k in range(len(previous))},
        compiler_params=pltpu.CompilerParams(vmem_limit_bytes=56 * 2 ** 20),
        cost_estimate=pl.CostEstimate(flops=ADAM_FLOPS * chunk * width, bytes_accessed=30 * chunk * width, transcendentals=0),
    )(rate, clip, grad, *states, *previous)


def place_kernel(spots, shard, *refs):
    count = len(spots)
    pieces = refs[:count]
    target, stored = refs[-2:]
    me, core, _, x_chip, y_chip, d_chip = places()
    chips = {'m': me // 2, 'x': x_chip, 'y': y_chip, 'd': d_chip}

    def store(k):
        chip, side, first_row = spots[k]
        owner = chips[chip] * 2 + (core if side == 0 else 1 - core)
        at = pl.multiple_of(owner * shard + first_row, 64)
        return pltpu.make_async_copy(pieces[k], target.at[pl.ds(at, pieces[k].shape[0])], stored.at[k])

    for k in range(count):
        store(k).start()
    for k in range(count):
        store(k).wait()


def place(shard, labelled, target, total_rows):
    spots = [spot for spot, _ in labelled]
    pieces = [piece for _, piece in labelled]
    width = pieces[0].shape[1]
    count = len(pieces)
    any_spec = pl.BlockSpec(memory_space=pl.ANY)
    previous = [] if target is None else [target]
    size = sum(piece.size for piece in pieces)
    return pl.pallas_call(
        functools.partial(place_kernel, spots, shard),
        out_shape=jax.ShapeDtypeStruct((total_rows, width), jnp.bfloat16),
        in_specs=[pl.BlockSpec(memory_space=pltpu.VMEM)] * count + [any_spec] * len(previous),
        out_specs=any_spec,
        scratch_shapes=[pltpu.SemaphoreType.DMA((count,))],
        input_output_aliases={count: 0} if previous else {},
        compiler_params=pltpu.CompilerParams(vmem_limit_bytes=PLACE_VMEM),
        cost_estimate=pl.CostEstimate(flops=PLACE_FLOPS * size, bytes_accessed=4 * size, transcendentals=0),
    )(*pieces, *previous)


def swap(value, bit):
    return lax.ppermute(value, 'dp', [(i, i ^ bit) for i in range(8)])


def solution(mesh):
    dev_count = mesh.shape['dp']

    def device_step(local_grads, master, mom_first, mom_second, learn_rate):
        shard = master.shape[0]
        total_rows = shard * dev_count
        rate = learn_rate.reshape(1)
        grad_shard, clip, head_rounded = reduce_grads(rate, local_grads, master, mom_first, mom_second)
        previous = []
        chunks = []
        for index in (*range(1, len(CHUNKS)), 0):
            first_row = sum(CHUNKS[:index])
            outs = adam_chunk(first_row, CHUNKS[index], rate, clip, grad_shard, (master, mom_first, mom_second), previous, total_rows)
            previous = list(outs[:3])
            chunks.append((first_row, outs[3]))
        chunks = [(0, head_rounded)] + chunks[:-1]
        near, far = [], []
        for index, (first_row, mine) in enumerate(chunks):
            from_x = swap(mine, 2)
            from_y = swap(mine, 4)
            from_d = swap(from_x, 4) if index % 2 == 0 else swap(from_y, 2)
            near += [(('m', 0, first_row), mine), (('m', 1, first_row), swap(mine, 1))]
            near += [(('x', 0, first_row), from_x), (('x', 1, first_row), swap(from_x, 1))]
            near += [(('y', 0, first_row), from_y), (('y', 1, first_row), swap(from_y, 1))]
            far += [(('d', 0, first_row), from_d), (('d', 1, first_row), swap(from_d, 1))]
        target = None
        for pair in range(len(CHUNKS) // 2):
            target = place(shard, near[12 * pair:12 * pair + 12], target, total_rows)
        last = len(CHUNKS) // 2 - 1
        for pair in range(last):
            target = place(shard, far[4 * pair:4 * pair + 4], target, total_rows)
        target = place(shard, far[4 * last::2], target, total_rows)
        target = place(shard, far[4 * last + 1::2], target, total_rows)
        return (*previous, target)

    return jax.shard_map(device_step, mesh=mesh, in_specs=(P('dp', None, None), P('dp', None), P('dp', None), P('dp', None), P()), out_specs=(P('dp', None), P('dp', None), P('dp', None), P(None, None)), check_vma=False)
```

```python
import functools

import jax
import jax.numpy as jnp
from jax import lax
from jax.experimental import pallas as pl
from jax.experimental.pallas import tpu as pltpu
from jax.sharding import PartitionSpec as P

LAYERS = 2
MIX_RANK = 32
DECAY_RANK = 64
ADAM_STEP = 10
MESH = pl.DeviceIdType.MESH
RAW = 3072
TILE = 384
PIECE = 192
SLAB = 64
ADAM_TILE = 192
ADAM_SLAB = 96
CHUNKS = (384, 384, 1152, 1152, 960, 960, 384, 384, 192, 192)
ADAM_FLOPS = 60
PLACE_FLOPS = 16
PLACE_VMEM = 24 * 2 ** 20


def layout_runs(model_width, total_rows):
    ffn_width = 7 * model_width // 2
    layer_rows = 6 * model_width + 2 * ffn_width + 16 + 10 * MIX_RANK + 2 * DECAY_RANK
    vocab_rows = (total_rows - LAYERS * layer_rows - 4) // 2
    base_rule = (1.0, 0.0)
    decay_rule = (1.0, 0.1)
    time_rule = (2.0, 0.0)
    pieces = [(vocab_rows, decay_rule)]
    for layer_idx in range(LAYERS):
        lead_rows = 12 if layer_idx == 0 else 10
        pieces = pieces + [(lead_rows + 10 * MIX_RANK, base_rule), (1, time_rule), (2 * DECAY_RANK, base_rule), (1, time_rule), (5 * model_width, decay_rule), (4, base_rule), (2 * ffn_width + model_width, decay_rule)]
    pieces = pieces + [(2, base_rule), (vocab_rows, decay_rule)]
    run_starts = []
    next_row = 0
    for run_len, run_rule in pieces:
        run_starts.append(next_row)
        next_row = next_row + run_len
    lr_values = [run_rule[0] for run_len, run_rule in pieces]
    decay_values = [run_rule[1] for run_len, run_rule in pieces]
    return run_starts, lr_values, decay_values


def places():
    me = lax.axis_index('dp')
    core = me % 2
    x = (me // 2) % 2
    y = me // 4
    x_chip = y * 2 + (1 - x)
    y_chip = (1 - y) * 2 + x
    d_chip = (1 - y) * 2 + (1 - x)
    return me, core, me + 1 - 2 * core, x_chip, y_chip, d_chip


def greet(partners):
    barrier = pltpu.get_barrier_semaphore()
    for partner in partners:
        pl.semaphore_signal(barrier, inc=1, device_id=(partner,), device_id_type=MESH)
    pl.semaphore_wait(barrier, len(partners))


def update_slab(row, total_rows, rate, clip_scale, grad, master, first, second, put):
    width = grad.shape[1]
    run_starts, lr_values, decay_values = layout_runs(width, total_rows)
    lr_factor = jnp.full(row.shape, lr_values[0], jnp.float32)
    decay = jnp.full(row.shape, decay_values[0], jnp.float32)
    for k in range(1, len(run_starts)):
        later = row >= run_starts[k]
        if lr_values[k] != lr_values[k - 1]:
            lr_factor = jnp.where(later, lr_values[k], lr_factor)
        if decay_values[k] != decay_values[k - 1]:
            decay = jnp.where(later, decay_values[k], decay)
    step_size = rate * lr_factor
    for lane in range(width // 128):
        cols = pl.ds(lane * 128, 128)
        clipped = grad[:, cols] * clip_scale
        old = master[:, cols]
        next_first = 0.9 * first[:, cols] + 0.1 * clipped
        next_second = 0.99 * second[:, cols] + 0.01 * (clipped * clipped)
        first_hat = next_first * (1.0 / (1.0 - 0.9 ** ADAM_STEP))
        second_hat = next_second * (1.0 / (1.0 - 0.99 ** ADAM_STEP))
        value = old - step_size * (first_hat / (jnp.sqrt(second_hat) + 1e-8) + decay * old)
        put(cols, value, next_first, next_second)


def adam_kernel(first_row, shard, total_rows, rate_ref, clip_ref, grad, master, first, second, *refs):
    new_master, new_first, new_second, rounded = refs[-4:]
    start = lax.axis_index('dp') * shard + first_row + pl.program_id(0) * ADAM_TILE
    rate = rate_ref[0]
    clip_scale = clip_ref[0:1, 0:1]

    @pl.loop(0, ADAM_TILE // ADAM_SLAB)
    def _(slab):
        at = pl.ds(pl.multiple_of(slab * ADAM_SLAB, ADAM_SLAB), ADAM_SLAB)
        row = start + slab * ADAM_SLAB + lax.broadcasted_iota(jnp.int32, (ADAM_SLAB, 128), 0)

        def put(cols, value, next_first, next_second):
            new_first[at, cols] = next_first
            new_second[at, cols] = next_second
            new_master[at, cols] = value
            rounded[at, cols] = value.astype(jnp.bfloat16)

        update_slab(row, total_rows, rate, clip_scale, grad.at[at], master.at[at], first.at[at], second.at[at], put)


def reduce_kernel(shard, rate_in, grads, master, first, second, total_ref, clip_out, rounded_ref, x_raw, y_raw, mate_raw,
                  relay, blocks, x_sum, y_sum, finals, head_grad, head_state, head_rounded, head_sem, rate_ref, clip_ref, squares, norm_mine, norm_all,
                  x_sent, y_sent, mate_sent, xs_sent, ys_sent, x_got, y_got, mate_got, xs_got, ys_got,
                  load_sem, store_sem, norm_sent, norm_got):
    half = shard // 2
    tiles = half // TILE
    me, core, mate, x_chip, y_chip, d_chip = places()
    mate_core = 1 - core
    x_peer, y_peer = x_chip * 2 + core, y_chip * 2 + core
    everyone = [d_chip * 2, d_chip * 2 + 1, x_chip * 2, x_chip * 2 + 1, y_chip * 2, y_chip * 2 + 1, mate]
    greet(everyone)
    head = [pltpu.make_async_copy(state.at[pl.ds(0, TILE)], head_state.at[k], head_sem.at[k]) for k, state in enumerate((master, first, second))]
    head.append(pltpu.make_async_copy(rate_in, rate_ref, head_sem.at[3]))

    def rows(tile):
        return pl.ds(pl.multiple_of(tile * TILE, TILE), TILE)

    def grad_tile(owner, part, tile):
        return grads.at[0, pl.ds(pl.multiple_of(owner * shard + part * half + tile * TILE, TILE), TILE), :]

    def remote(src, dst, sent, got, device):
        return pltpu.make_async_remote_copy(src_ref=src, dst_ref=dst, send_sem=sent, recv_sem=got, device_id=(device,), device_id_type=MESH)

    def raw_rows(block):
        return pl.ds(pl.multiple_of(block * RAW, RAW), RAW)

    def grad_block(owner, part, block):
        return grads.at[0, pl.ds(pl.multiple_of(owner * shard + part * half + block * RAW, TILE), RAW), :]

    def send_raw(stage, block):
        x_owner = d_chip if stage == 0 else x_chip
        y_owner = d_chip if stage == 0 else y_chip
        for dest in range(2):
            remote(grad_block(x_owner * 2 + dest, 0, block), x_raw.at[stage, core, raw_rows(block)], x_sent.at[block], x_got.at[stage, core, block], x_chip * 2 + dest).start()
            remote(grad_block(y_owner * 2 + dest, 1, block), y_raw.at[stage, core, raw_rows(block)], y_sent.at[block], y_got.at[stage, core, block], y_chip * 2 + dest).start()
        first = y_chip * 2 + mate_core if stage == 0 else mate
        second = x_chip * 2 + mate_core if stage == 0 else mate
        remote(grad_block(first, 0, block), mate_raw.at[2 * stage, raw_rows(block)], mate_sent.at[block], mate_got.at[2 * stage, block], mate).start()
        remote(grad_block(second, 1, block), mate_raw.at[2 * stage + 1, raw_rows(block)], mate_sent.at[block], mate_got.at[2 * stage + 1, block], mate).start()

    def arrived(ref, sem):
        remote(ref, ref, sem, sem, mate).wait_recv()

    def wait_raw(stage, tile):
        @pl.when(tile % (RAW // TILE) == 0)
        def _():
            block = tile // (RAW // TILE)
            for source in range(2):
                arrived(x_raw.at[stage, source, raw_rows(block)], x_got.at[stage, source, block])
                arrived(y_raw.at[stage, source, raw_rows(block)], y_got.at[stage, source, block])
            for part in range(2):
                arrived(mate_raw.at[2 * stage + part, raw_rows(block)], mate_got.at[2 * stage + part, block])

    def loads(stage, tile):
        owners = (y_peer, x_peer) if stage == 0 else (me, me)
        out = []
        for part in range(2):
            far = x_raw if part == 0 else y_raw
            sources = [grad_tile(owners[part], part, tile), mate_raw.at[2 * stage + part, rows(tile)], far.at[stage, 0, rows(tile)], far.at[stage, 1, rows(tile)]]
            for k, source in enumerate(sources):
                out.append(pltpu.make_async_copy(source, blocks.at[part, k], load_sem.at[part, k]))
        return out

    @pl.loop(0, half // RAW)
    def _(block):
        send_raw(0, block)

    @pl.loop(0, tiles)
    def _(tile):
        @pl.when(tile % (RAW // TILE) == 0)
        def _():
            send_raw(1, tile // (RAW // TILE))

        wait_raw(0, tile)
        copies = loads(0, tile)
        for copy in copies:
            copy.start()
        for copy in copies:
            copy.wait()
        for piece in range(TILE // PIECE):
            here = pl.ds(piece * PIECE, PIECE)
            for part in range(2):
                @pl.loop(piece * PIECE // SLAB, (piece + 1) * PIECE // SLAB)
                def _(slab):
                    at = pl.ds(pl.multiple_of(slab * SLAB, SLAB), SLAB)
                    parts = [blocks[part, k, at, :].astype(jnp.float32) for k in range(4)]
                    relay[part, tile, at, :] = (parts[0] + parts[1]) + (parts[2] + parts[3])

                if part == 0:
                    remote(relay.at[0, tile, here], y_sum.at[tile, here], ys_sent.at[tile], ys_got.at[tile, piece], y_peer).start()
                else:
                    remote(relay.at[1, tile, here], x_sum.at[tile, here], xs_sent.at[tile], xs_got.at[tile, piece], x_peer).start()

    for copy in head:
        copy.start()
    squares[...] = jnp.zeros_like(squares)

    def total_tile(part, tile):
        return total_ref.at[pl.ds(pl.multiple_of(part * half + tile * TILE, TILE), TILE), :]

    @pl.loop(0, tiles)
    def _(tile):
        wait_raw(1, tile)
        copies = loads(1, tile)
        for copy in copies:
            copy.start()
        for copy in copies:
            copy.wait()

        @pl.when(tile > 0)
        def _():
            for part in range(2):
                pltpu.make_async_copy(finals.at[part], total_tile(part, tile), store_sem.at[part]).wait()

        for piece in range(TILE // PIECE):
            for part in range(2):
                far_sum, far_got = (y_sum, x_sum)[part], (ys_got, xs_got)[part]
                arrived(far_sum.at[tile, pl.ds(piece * PIECE, PIECE)], far_got.at[tile, piece])

                @pl.loop(piece * PIECE // SLAB, (piece + 1) * PIECE // SLAB)
                def _(slab):
                    at = pl.ds(pl.multiple_of(slab * SLAB, SLAB), SLAB)
                    parts = [blocks[part, k, at, :].astype(jnp.float32) for k in range(4)]
                    mean = ((parts[0] + parts[1]) + (parts[2] + parts[3]) + far_sum[tile, at, :]) * 0.125
                    finals[part, at, :] = mean
                    if part == 0:
                        @pl.when(tile == 0)
                        def _():
                            head_grad[at, :] = mean
                    squares[...] += jnp.sum((mean * mean).reshape(SLAB // 8, 8, mean.shape[1]), axis=0)

        for part in range(2):
            pltpu.make_async_copy(finals.at[part], total_tile(part, tile), store_sem.at[part]).start()

    width = squares.shape[1]
    packed = squares[:, 0:128]
    for lane in range(1, width // 128):
        packed = packed + squares[:, lane * 128:lane * 128 + 128]
    norm_mine[...] = packed
    norm_all[me] = packed
    for k, partner in enumerate(everyone):
        remote(norm_mine, norm_all.at[me], norm_sent.at[k], norm_got.at[me], partner).start()
    for part in range(2):
        pltpu.make_async_copy(finals.at[part], total_tile(part, 0), store_sem.at[part]).wait()
    for copy in head:
        copy.wait()
    for partner in everyone:
        arrived(norm_all.at[partner], norm_got.at[partner])
    squared = norm_all[0]
    for k in range(1, 8):
        squared = squared + norm_all[k]
    norm = jnp.sqrt(jnp.sum(squared, keepdims=True))
    clip_scale = jnp.minimum(1.0, 1.0 / (norm + 1e-6))
    clip_ref[...] = jnp.broadcast_to(clip_scale, clip_ref.shape)
    clip_copy = pltpu.make_async_copy(clip_ref, clip_out, head_sem.at[4])

    def head_slab(slab):
        at = pl.ds(pl.multiple_of(slab * ADAM_SLAB, ADAM_SLAB), ADAM_SLAB)
        row = me * shard + slab * ADAM_SLAB + lax.broadcasted_iota(jnp.int32, (ADAM_SLAB, 128), 0)

        def put(cols, value, next_first, next_second):
            head_rounded[at, cols] = value.astype(jnp.bfloat16)

        update_slab(row, 8 * shard, rate_ref[0], clip_ref[0:1, 0:1], head_grad.at[at], head_state.at[0, at], head_state.at[1, at], head_state.at[2, at], put)

    for piece in range(TILE // PIECE):
        pl.loop(piece * PIECE // ADAM_SLAB, (piece + 1) * PIECE // ADAM_SLAB)(head_slab)
        if piece == 0:
            clip_copy.start()
        here = pl.ds(piece * PIECE, PIECE)
        pltpu.make_async_copy(head_rounded.at[here], rounded_ref.at[here], head_sem.at[5 + piece]).start()

    for k, partner in enumerate(everyone):
        remote(norm_mine, norm_mine, norm_sent.at[k], norm_sent.at[k], partner).wait_send()

    @pl.loop(0, half // RAW)
    def _(block):
        for ref, sem in ((x_raw.at[:, :, raw_rows(block)], x_sent), (y_raw.at[:, :, raw_rows(block)], y_sent), (mate_raw.at[:, raw_rows(block)], mate_sent)):
            remote(ref, ref, sem.at[block], sem.at[block], mate).wait_send()

    @pl.loop(0, tiles)
    def _(tile):
        for ref, sem in ((x_sum.at[tile], xs_sent), (y_sum.at[tile], ys_sent)):
            remote(ref, ref, sem.at[tile], sem.at[tile], mate).wait_send()

    clip_copy.wait()
    for piece in range(TILE // PIECE):
        here = pl.ds(piece * PIECE, PIECE)
        pltpu.make_async_copy(head_rounded.at[here], rounded_ref.at[here], head_sem.at[5 + piece]).wait()


def reduce_grads(rate, local_grads, master, first, second):
    shard = master.shape[0]
    width = local_grads.shape[2]
    half = shard // 2
    tiles = half // TILE
    blocks = half // RAW
    any_spec = pl.BlockSpec(memory_space=pl.ANY)
    bf16, f32 = jnp.bfloat16, jnp.float32
    dma = pltpu.SemaphoreType.DMA
    outs = pl.pallas_call(
        functools.partial(reduce_kernel, shard),
        out_shape=[
            jax.ShapeDtypeStruct((shard, width), f32),
            jax.ShapeDtypeStruct((8, 128), f32),
            jax.ShapeDtypeStruct((TILE, width), bf16),
            jax.ShapeDtypeStruct((2, 2, half, width), bf16),
            jax.ShapeDtypeStruct((2, 2, half, width), bf16),
            jax.ShapeDtypeStruct((4, half, width), bf16),
        ],
        in_specs=[any_spec] * 5,
        out_specs=[any_spec] * 6,
        scratch_shapes=[
            pltpu.VMEM((2, tiles, TILE, width), f32),
            pltpu.VMEM((2, 4, TILE, width), bf16),
            pltpu.VMEM((tiles, TILE, width), f32),
            pltpu.VMEM((tiles, TILE, width), f32),
            pltpu.VMEM((2, TILE, width), f32),
            pltpu.VMEM((TILE, width), f32),
            pltpu.VMEM((3, TILE, width), f32),
            pltpu.VMEM((TILE, width), bf16),
            dma((5 + TILE // PIECE,)),
            pltpu.SMEM((1,), f32),
            pltpu.VMEM((8, 128), f32),
            pltpu.VMEM((8, width), f32),
            pltpu.VMEM((8, 128), f32),
            pltpu.VMEM((8, 8, 128), f32),
            dma((blocks,)), dma((blocks,)), dma((blocks,)), dma((tiles,)), dma((tiles,)),
            dma((2, 2, blocks)), dma((2, 2, blocks)), dma((4, blocks)), dma((tiles, TILE // PIECE)), dma((tiles, TILE // PIECE)),
            dma((2, 4)), dma((2,)), dma((7,)), dma((8,)),
        ],
        compiler_params=pltpu.CompilerParams(collective_id=0, has_side_effects=True, vmem_limit_bytes=56 * 2 ** 20),
        name='reduce_grads',
    )(rate, local_grads, master, first, second)
    return outs[:3]


def adam_chunk(first_row, chunk, rate, clip, grad, states, previous, total_rows):
    shard, width = grad.shape
    block = pl.BlockSpec((ADAM_TILE, width), lambda step: (first_row // ADAM_TILE + step, 0))
    own = pl.BlockSpec((ADAM_TILE, width), lambda step: (step, 0))
    any_spec = pl.BlockSpec(memory_space=pl.ANY)
    smem = pl.BlockSpec(memory_space=pltpu.SMEM)
    vmem = pl.BlockSpec((8, 128), lambda step: (0, 0))
    full = jax.ShapeDtypeStruct((shard, width), jnp.float32)
    return pl.pallas_call(
        functools.partial(adam_kernel, first_row, shard, total_rows),
        grid=(chunk // ADAM_TILE,),
        out_shape=[full] * 3 + [jax.ShapeDtypeStruct((chunk, width), jnp.bfloat16)],
        in_specs=[smem, vmem] + [block] * 4 + [any_spec] * len(previous),
        out_specs=[block] * 3 + [own],
        input_output_aliases={6 + k: k for k in range(len(previous))},
        compiler_params=pltpu.CompilerParams(vmem_limit_bytes=56 * 2 ** 20),
        cost_estimate=pl.CostEstimate(flops=ADAM_FLOPS * chunk * width, bytes_accessed=30 * chunk * width, transcendentals=0),
    )(rate, clip, grad, *states, *previous)


def place_kernel(spots, shard, *refs):
    count = len(spots)
    pieces = refs[:count]
    target, stored = refs[-2:]
    me, core, _, x_chip, y_chip, d_chip = places()
    chips = {'m': me // 2, 'x': x_chip, 'y': y_chip, 'd': d_chip}

    def store(k):
        chip, side, first_row = spots[k]
        owner = chips[chip] * 2 + (core if side == 0 else 1 - core)
        at = pl.multiple_of(owner * shard + first_row, 64)
        return pltpu.make_async_copy(pieces[k], target.at[pl.ds(at, pieces[k].shape[0])], stored.at[k])

    for k in range(count):
        store(k).start()
    for k in range(count):
        store(k).wait()


def place(shard, labelled, target, total_rows):
    spots = [spot for spot, _ in labelled]
    pieces = [piece for _, piece in labelled]
    width = pieces[0].shape[1]
    count = len(pieces)
    any_spec = pl.BlockSpec(memory_space=pl.ANY)
    previous = [] if target is None else [target]
    size = sum(piece.size for piece in pieces)
    return pl.pallas_call(
        functools.partial(place_kernel, spots, shard),
        out_shape=jax.ShapeDtypeStruct((total_rows, width), jnp.bfloat16),
        in_specs=[pl.BlockSpec(memory_space=pltpu.VMEM)] * count + [any_spec] * len(previous),
        out_specs=any_spec,
        scratch_shapes=[pltpu.SemaphoreType.DMA((count,))],
        input_output_aliases={count: 0} if previous else {},
        compiler_params=pltpu.CompilerParams(vmem_limit_bytes=PLACE_VMEM),
        cost_estimate=pl.CostEstimate(flops=PLACE_FLOPS * size, bytes_accessed=4 * size, transcendentals=0),
    )(*pieces, *previous)


def swap(value, bit):
    return lax.ppermute(value, 'dp', [(i, i ^ bit) for i in range(8)])


def solution(mesh):
    dev_count = mesh.shape['dp']

    def device_step(local_grads, master, mom_first, mom_second, learn_rate):
        shard = master.shape[0]
        total_rows = shard * dev_count
        rate = learn_rate.reshape(1)
        grad_shard, clip, head_rounded = reduce_grads(rate, local_grads, master, mom_first, mom_second)
        previous = []
        chunks = []
        for index in (*range(1, len(CHUNKS)), 0):
            first_row = sum(CHUNKS[:index])
            outs = adam_chunk(first_row, CHUNKS[index], rate, clip, grad_shard, (master, mom_first, mom_second), previous, total_rows)
            previous = list(outs[:3])
            chunks.append((first_row, outs[3]))
        chunks = [(0, head_rounded)] + chunks[:-1]
        near, far = [], []
        for index, (first_row, mine) in enumerate(chunks):
            from_x = swap(mine, 2)
            from_y = swap(mine, 4)
            from_d = swap(from_x, 4) if index % 2 == 0 else swap(from_y, 2)
            near += [(('m', 0, first_row), mine), (('m', 1, first_row), swap(mine, 1))]
            near += [(('x', 0, first_row), from_x), (('x', 1, first_row), swap(from_x, 1))]
            near += [(('y', 0, first_row), from_y), (('y', 1, first_row), swap(from_y, 1))]
            far += [(('d', 0, first_row), from_d), (('d', 1, first_row), swap(from_d, 1))]
        target = None
        for pair in range(len(CHUNKS) // 2):
            target = place(shard, near[12 * pair:12 * pair + 12], target, total_rows)
        last = len(CHUNKS) // 2 - 1
        for pair in range(last):
            target = place(shard, far[4 * pair:4 * pair + 4], target, total_rows)
        target = place(shard, far[4 * last::2], target, total_rows)
        target = place(shard, far[4 * last + 1::2], target, total_rows)
        return (*previous, target)

    return jax.shard_map(device_step, mesh=mesh, in_specs=(P('dp', None, None), P('dp', None), P('dp', None), P('dp', None), P()), out_specs=(P('dp', None), P('dp', None), P('dp', None), P(None, None)), check_vma=False)
```
